8 devices in a mesh: tp: 4 (over z, y, x), pool: 2 (over core).
Axes of the slice: x: 2, y: 2, z: 1, core: 2. Of those that a mesh axis runs over, the one named last changes fastest.
Arguments:
- base_up: bfloat16 [1, 8192, 32768], P(None, None, 'tp')
- base_down: bfloat16 [1, 32768, 8192], P(None, 'tp')
- up_left: float32 [2, 1, 8192, 128], P('pool', None, 'tp')
- up_right: float32 [2, 1, 128, 32768], P('pool', None, None, 'tp')
- down_left: float32 [2, 1, 32768, 128], P('pool', None, 'tp')
- down_right: float32 [2, 1, 128, 8192], P('pool', None, None, 'tp')
- grad_up_left: float32 [2, 1, 8192, 128], P('pool', None, 'tp')
- grad_up_right: float32 [2, 1, 128, 32768], P('pool', None, None, 'tp')
- grad_down_left: float32 [2, 1, 32768, 128], P('pool', None, 'tp')
- grad_down_right: float32 [2, 1, 128, 8192], P('pool', None, None, 'tp')
- learn_rate: float32 [1], replicated
- prompts: bfloat16 [2, 2048, 8192], P('pool')
Outputs:
- output 1: float32 [2, 1, 8192, 128], P('pool', None, 'tp')
- output 2: float32 [2, 1, 128, 32768], P('pool', None, None, 'tp')
- output 3: float32 [2, 1, 32768, 128], P('pool', None, 'tp')
- output 4: float32 [2, 1, 128, 8192], P('pool', None, None, 'tp')
- output 5: bfloat16 [2, 2048, 8192], P('pool')
All inputs are finite; a program needn't handle non-finite values.
Results may differ from the reference program's by a relative error of at most 0.00188.
Values are sent between devices in bfloat16 or wider.
A program may use at most 1.5 GiB of HBM per device.

```python
import jax
import jax.numpy as jnp
from jax import lax

LAYERS = 1
D = 8192
FF = 32768
RANK = 128
TOKENS = 2048
REPLICAS = 1
TP_SIZE = 4


def trainer_slots(draw_key, block_shape, std_scale):
    real_part = jax.random.normal(draw_key, (REPLICAS,) + block_shape, jnp.float32) * std_scale
    return jnp.concatenate([real_part, jnp.zeros_like(real_part)], axis=0)


def setup_inputs(seed: int = 0) -> dict:
    key_list = jax.random.split(jax.random.key(seed), 12)
    d_block = D // REPLICAS
    f_block = FF // REPLICAS
    left_scale = RANK ** -0.5
    up_scale = (0.5 / D) ** 0.5
    down_scale = (1.0 / (LAYERS * FF)) ** 0.5
    base_up = (jax.random.normal(key_list[0], (LAYERS, D, FF), jnp.float32) * up_scale).astype(jnp.bfloat16)
    base_down = (jax.random.normal(key_list[1], (LAYERS, FF, D), jnp.float32) * down_scale).astype(jnp.bfloat16)
    up_left = trainer_slots(key_list[2], (LAYERS, d_block, RANK), left_scale)
    up_right = trainer_slots(key_list[3], (LAYERS, RANK, f_block), up_scale)
    down_left = trainer_slots(key_list[4], (LAYERS, f_block, RANK), left_scale)
    down_right = trainer_slots(key_list[5], (LAYERS, RANK, d_block), down_scale)
    grad_up_left = trainer_slots(key_list[6], (LAYERS, d_block, RANK), left_scale)
    grad_up_right = trainer_slots(key_list[7], (LAYERS, RANK, f_block), up_scale)
    grad_down_left = trainer_slots(key_list[8], (LAYERS, f_block, RANK), left_scale)
    grad_down_right = trainer_slots(key_list[9], (LAYERS, RANK, d_block), down_scale)
    learn_rate = jax.random.uniform(key_list[10], (1,), jnp.float32, 0.05, 0.25)
    real_prompts = jax.random.normal(key_list[11], (REPLICAS, TOKENS, D), jnp.float32).astype(jnp.bfloat16)
    prompts = jnp.concatenate([jnp.zeros_like(real_prompts), real_prompts], axis=0)
    return {'base_up': base_up, 'base_down': base_down, 'up_left': up_left, 'up_right': up_right, 'down_left': down_left, 'down_right': down_right, 'grad_up_left': grad_up_left, 'grad_up_right': grad_up_right, 'grad_down_left': grad_down_left, 'grad_down_right': grad_down_right, 'learn_rate': learn_rate, 'prompts': prompts}


def unslot_left(slot_arr):
    real_part = slot_arr[:REPLICAS].reshape(REPLICAS, LAYERS, TP_SIZE, -1, RANK)
    return real_part.transpose(1, 2, 0, 3, 4).reshape(LAYERS, -1, RANK)


def unslot_right(slot_arr):
    real_part = slot_arr[:REPLICAS].reshape(REPLICAS, LAYERS, RANK, TP_SIZE, -1)
    return real_part.transpose(1, 2, 3, 0, 4).reshape(LAYERS, RANK, -1)


def reference(base_up, base_down, up_left, up_right, down_left, down_right, grad_up_left, grad_up_right, grad_down_left, grad_down_right, learn_rate, prompts):
    step_size = learn_rate[0]
    new_up_left = up_left - step_size * grad_up_left
    new_up_right = up_right - step_size * grad_up_right
    new_down_left = down_left - step_size * grad_down_left
    new_down_right = down_right - step_size * grad_down_right
    stacked = (base_up, base_down,
               unslot_left(new_up_left).astype(jnp.bfloat16),
               unslot_right(new_up_right).astype(jnp.bfloat16),
               unslot_left(new_down_left).astype(jnp.bfloat16),
               unslot_right(new_down_right).astype(jnp.bfloat16))

    def layer_step(hidden, params):
        w_up_base, w_down_base, left_up, right_up, left_down, right_down = params
        delta_up = jnp.dot(left_up, right_up, preferred_element_type=jnp.float32).astype(jnp.bfloat16)
        delta_down = jnp.dot(left_down, right_down, preferred_element_type=jnp.float32).astype(jnp.bfloat16)
        w_up = (w_up_base.astype(jnp.float32) + delta_up.astype(jnp.float32)).astype(jnp.bfloat16)
        w_down = (w_down_base.astype(jnp.float32) + delta_down.astype(jnp.float32)).astype(jnp.bfloat16)
        pre_act = jnp.dot(hidden, w_up, preferred_element_type=jnp.float32)
        gelu_out = jax.nn.gelu(pre_act, approximate=True).astype(jnp.bfloat16)
        down_out = jnp.dot(gelu_out, w_down, preferred_element_type=jnp.float32)
        return (hidden.astype(jnp.float32) + down_out).astype(jnp.bfloat16), None

    start_rows = prompts[REPLICAS:].reshape(REPLICAS * TOKENS, D)
    final_rows, _ = lax.scan(layer_step, start_rows, stacked)
    gen_out = final_rows.reshape(REPLICAS, TOKENS, D)
    hidden_out = jnp.concatenate([jnp.zeros_like(gen_out), gen_out], axis=0)
    return (new_up_left, new_up_right, new_down_left, new_down_right, hidden_out)
```

```python
import jax
import jax.numpy as jnp
from jax import lax
from jax.sharding import PartitionSpec as P

CHUNKS = 4


def solution(mesh):
    left_spec = P('pool', None, 'tp', None)
    right_spec = P('pool', None, None, 'tp')
    prompt_spec = P('pool', None, None)

    def local_step(base_up, base_down, up_left, up_right, down_left, down_right, grad_up_left, grad_up_right, grad_down_left, grad_down_right, learn_rate, prompts):
        step_size = learn_rate[0]
        core = lax.axis_index('pool')
        new_up_left = up_left - step_size * grad_up_left
        new_up_right = up_right - step_size * grad_up_right
        new_down_left = down_left - step_size * grad_down_left
        new_down_right = down_right - step_size * grad_down_right
        own = tuple(part[0, 0].astype(jnp.bfloat16) for part in (new_up_left, new_up_right, new_down_left, new_down_right))
        sent = lax.ppermute(own, 'pool', [(0, 1)])
        parts = tuple(jnp.where(core == 0, a, b) for a, b in zip(own, sent))
        up_left_full = lax.all_gather(parts[0], 'tp', axis=0, tiled=True)
        down_right_full = lax.all_gather(parts[3], 'tp', axis=1, tiled=True)
        half = base_up.shape[2] // 2
        up_cols = lax.dynamic_slice_in_dim(parts[1], core * half, half, 1)
        down_rows = lax.dynamic_slice_in_dim(parts[2], core * half, half, 0)
        delta_up = jnp.dot(up_left_full, up_cols, preferred_element_type=jnp.float32).astype(jnp.bfloat16)
        delta_down = jnp.dot(down_rows, down_right_full, preferred_element_type=jnp.float32).astype(jnp.bfloat16)
        w_up = lax.dynamic_slice_in_dim(base_up[0], core * half, half, 1) + delta_up
        w_down = lax.dynamic_slice_in_dim(base_down[0], core * half, half, 0) + delta_down
        tokens = prompts.shape[1]
        rows = tokens // CHUNKS
        shard = rows // 8
        me = lax.axis_index('tp') * 2 + core
        outs = []
        for c in range(CHUNKS):
            mine = lax.slice_in_dim(prompts[0], c * rows, (c + 1) * rows, axis=0)
            got = lax.ppermute(mine, 'pool', [(1, 0)])
            x = jnp.where(core == 1, mine, got)
            pre_act = jnp.dot(x, w_up, preferred_element_type=jnp.float32)
            u = jax.nn.gelu(pre_act, approximate=True).astype(jnp.bfloat16)
            part = jnp.dot(u, w_down, preferred_element_type=jnp.float32)
            summed = lax.psum_scatter(part, ('tp', 'pool'), scatter_dimension=0, tiled=True)
            res = lax.dynamic_slice_in_dim(x, me * shard, shard, 0)
            h = (res.astype(jnp.float32) + summed).astype(jnp.bfloat16)
            outs.append(lax.all_gather(h, ('tp', 'pool'), axis=0, tiled=True))
        hidden = jnp.concatenate(outs, axis=0)
        hidden_out = jnp.where(core == 1, hidden, jnp.zeros_like(hidden))[None]
        return new_up_left, new_up_right, new_down_left, new_down_right, hidden_out

    return jax.shard_map(local_step, mesh=mesh,
                         in_specs=(P(None, None, 'tp'), P(None, 'tp', None), left_spec, right_spec, left_spec, right_spec, left_spec, right_spec, left_spec, right_spec, P(None), prompt_spec),
                         out_specs=(left_spec, right_spec, left_spec, right_spec, prompt_spec),
                         check_vma=False)
```

```python
import functools

import jax
import jax.numpy as jnp
from jax import lax
from jax.experimental import pallas as pl
from jax.experimental.pallas import tpu as pltpu
from jax.sharding import PartitionSpec as P

CHUNK = 512
TILE = 256
RING = 3
LAG = (2, 4, 7, 23)
BF16 = jnp.bfloat16
F32 = jnp.float32
MESH = pl.DeviceIdType.MESH


def mlp_kernel(dims, base_up, base_dn, a_up, b_up, a_dn, b_dn, prompts, hid, wm,
               x, u, wb, aup, bup, adn, bdn, pb, rx0, s1, rx1, rx2, ob, res,
               wsem, osem, lsem, asend, arecv, xsem, s0, r0, ss1, rs1, ss2, rs2, ss3, rs3, ss4, ss5, fsem,
               xfree, cr1, cr2, cr3):
    m, nc, nb, d, fh, w = dims
    total = nc * nb
    ring = nb
    halves = w // TILE
    mh, mq, me = m // 2, m // 4, m // 8
    d4 = d // 4
    t = lax.axis_index('tp')
    c = lax.axis_index('pool')
    xb, yb = t % 2, t // 2
    near_x, near_y = t + 1 - 2 * xb, t + 2 - 4 * yb
    b1 = (1 - c) * xb + c * yb
    b2 = c * xb + (1 - c) * yb
    p1 = (1 - c) * near_x + c * near_y
    p2 = c * near_x + (1 - c) * near_y

    def rows(start, size):
        return pl.ds(pl.multiple_of(start, size), size)

    def remote(src, dst, send, recv, device):
        return pltpu.make_async_remote_copy(src_ref=src, dst_ref=dst, send_sem=send, recv_sem=recv,
                                            device_id=device, device_id_type=MESH)

    def base_loads(r, slot):
        @pl.when(r < nb)
        def _():
            pltpu.make_async_copy(base_up.at[0, :, rows(c * fh + r * TILE, TILE)], wb.at[slot], wsem.at[slot]).start()

        @pl.when(r >= nb)
        def _():
            for h in range(halves):
                pltpu.make_async_copy(base_dn.at[0, rows(c * fh, fh), rows((r - nb) * w + h * TILE, TILE)],
                                      wb.at[slot, pl.ds(h * fh, fh), :], wsem.at[slot]).start()

    def merged_load(r, slot):
        return pltpu.make_async_copy(wm.at[r], wb.at[slot], wsem.at[slot])

    def merged_store(r, slot):
        return pltpu.make_async_copy(wb.at[slot], wm.at[r], osem.at[slot])

    piece = min(512, fh)

    def merge_up(slot, j):
        right = bup[:, rows(j * TILE, TILE)]
        for q in range(d // piece):
            part = pl.ds(q * piece, piece)
            delta = jnp.dot(aup[part, :], right, preferred_element_type=F32).astype(BF16)
            wb[slot, part, :] = wb[slot, part, :] + delta

    def merge_dn(slot, i):
        for h in range(halves):
            right = bdn[:, rows(i * w + h * TILE, TILE)]
            for q in range(fh // piece):
                delta = jnp.dot(adn[pl.ds(q * piece, piece), :], right, preferred_element_type=F32).astype(BF16)
                part = pl.ds(h * fh + q * piece, piece)
                wb[slot, part, :] = wb[slot, part, :] + delta

    def dot_up(slot, j):
        pre = jnp.dot(x[...], wb[slot], preferred_element_type=F32)
        u[:, rows(j * TILE, TILE)] = jax.nn.gelu(pre, approximate=True).astype(BF16)

    def dot_dn(slot, buf):
        for h in range(halves):
            pb[buf, :, pl.ds(h * TILE, TILE)] = jnp.dot(u[...], wb[slot, pl.ds(h * fh, fh), :],
                                                        preferred_element_type=F32)

    def swap(g):
        return remote(pb.at[g % 2, rows((1 - c) * mh, mh), :], rx0.at[g % 4], s0.at[g % 2], r0.at[g % 4], (t, 1 - c))

    def first(g):
        return remote(s1.at[g % ring, rows((1 - b1) * mq, mq), :], rx1.at[g % ring],
                      ss1.at[g % ring], rs1.at[g % ring], (p1, c))

    def second(g):
        return remote(s1.at[g % ring, rows(b1 * mq + (1 - b2) * me, me), :], rx2.at[g % ring],
                      ss2.at[g % ring], rs2.at[g % ring], (p2, c))

    def gather(g):
        half = ob.at[g % ring, rows(b2 * me, me), :]
        return remote(half, half, ss3.at[g % ring], rs3.at[g % ring], (p2, c))

    def final_place(g):
        return hid.at[rows((g // nb) * m + c * mh + b1 * mq, mq), rows((g % nb) * w, w)]

    def final_far(g):
        return remote(ob.at[g % ring], final_place(g), ss4.at[g % ring], fsem.at[1 + c], (p1, 1))

    def final_near(g):
        return remote(ob.at[g % ring], final_place(g), ss5.at[g % ring], fsem.at[0], (t, 1))

    def final_local(g):
        return pltpu.make_async_copy(ob.at[g % ring], final_place(g), ss5.at[g % ring])

    def stage_a(g):
        slot = g % ring
        swap(g).wait_send()
        swap(g).wait_recv()
        s1[slot] = pb[g % 2, rows(c * mh, mh), :] + rx0[g % 4]

        @pl.when(g >= ring)
        def _():
            pl.semaphore_wait(cr1, 1)
        first(g).start()

    def stage_b(g):
        slot = g % ring
        keep = rows(b1 * mq, mq)
        first(g).wait_recv()
        s1[slot, keep, :] = s1[slot, keep, :] + rx1[slot]

        @pl.when(g + ring < total)
        def _():
            pl.semaphore_signal(cr1, inc=1, device_id=(p1, c), device_id_type=MESH)

        @pl.when(g >= ring)
        def _():
            pl.semaphore_wait(cr2, 1)
        second(g).start()

    def stage_c(g):
        slot = g % ring
        keep = rows(b1 * mq + b2 * me, me)
        second(g).wait_recv()
        first(g).wait_send()
        held = res[(g // nb) % 2, :, rows((g % nb) * w, w)].astype(F32)
        ob[slot, rows(b2 * me, me), :] = (held + (s1[slot, keep, :] + rx2[slot])).astype(BF16)

        @pl.when(g + ring < total)
        def _():
            pl.semaphore_signal(cr2, inc=1, device_id=(p2, c), device_id_type=MESH)

        @pl.when(g >= ring)
        def _():
            pl.semaphore_wait(cr3, 1)
        gather(g).start()

    def stage_d(g):
        gather(g).wait_recv()
        second(g).wait_send()
        final_far(g).start()

        @pl.when(c == 0)
        def _():
            final_near(g).start()

        @pl.when(c == 1)
        def _():
            final_local(g).start()

    def stage_e(g):
        gather(g).wait_send()
        final_far(g).wait_send()

        @pl.when(c == 0)
        def _():
            final_near(g).wait_send()

        @pl.when(c == 1)
        def _():
            final_local(g).wait()

        @pl.when(g + ring < total)
        def _():
            pl.semaphore_signal(cr3, inc=1, device_id=(p2, c), device_id_type=MESH)

    def stages(s):
        before = s - 1
        r = before % (2 * nb)

        @pl.when((r >= nb) & (before < 2 * nb * nc))
        def _():
            stage_a((before // (2 * nb)) * nb + r - nb)
        for lag, stage in zip(LAG, (stage_b, stage_c, stage_d, stage_e)):
            late = s - nb - lag

            @pl.when((late >= 0) & (late % 2 == 0) & (late < 2 * total))
            def _():
                stage(late // 2)

    def x_load(k):
        return pltpu.make_async_copy(prompts.at[0, rows(k * m, m), :], x, xsem.at[0])

    def x_send():
        return remote(x, x, xsem.at[1], xsem.at[2], (t, 0))

    def keep_rows(k):
        res[k % 2] = x[rows(c * mh + b1 * mq + b2 * me, me), :]

    def up_piece(owner):
        return aup.at[rows(owner * d4, d4), :]

    def dn_piece(owner):
        return bdn.at[:, rows(owner * d4, d4)]

    others = (near_x, near_y, 3 - t)

    def up_out(n):
        return remote(a_up, up_piece(t), asend.at[n], arecv.at[t], (others[n], 0))

    def dn_out(n):
        return remote(b_dn, dn_piece(t), asend.at[3 + n], arecv.at[4 + t], (others[n], 0))

    def up_in(owner):
        return remote(up_piece(owner), up_piece(owner), asend.at[6], arecv.at[owner], (t, 1))

    def dn_in(owner):
        return remote(dn_piece(owner), dn_piece(owner), asend.at[7], arecv.at[4 + owner], (t, 1))

    def pass_up(n):
        return remote(up_piece(others[n]), up_piece(others[n]), asend.at[8 + n], arecv.at[others[n]], (t, 1))

    def pass_dn(n):
        return remote(dn_piece(others[n]), dn_piece(others[n]), asend.at[11 + n], arecv.at[4 + others[n]], (t, 1))

    own = (
        lambda: remote(a_up, up_piece(t), asend.at[14], arecv.at[t], (t, 1)),
        lambda: remote(b_up.at[:, pl.ds(fh, fh)], bup, asend.at[15], arecv.at[8], (t, 1)),
        lambda: remote(a_dn.at[pl.ds(fh, fh), :], adn, asend.at[16], arecv.at[9], (t, 1)),
        lambda: remote(b_dn, dn_piece(t), asend.at[17], arecv.at[4 + t], (t, 1)),
    )
    local = (
        lambda: pltpu.make_async_copy(a_up, up_piece(t), lsem.at[0]),
        lambda: pltpu.make_async_copy(b_up.at[:, pl.ds(0, fh)], bup, lsem.at[1]),
        lambda: pltpu.make_async_copy(a_dn.at[pl.ds(0, fh), :], adn, lsem.at[2]),
        lambda: pltpu.make_async_copy(b_dn, dn_piece(t), lsem.at[3]),
    )

    base_loads(0, 0)
    base_loads(1, 1)

    @pl.when(c == 0)
    def _():
        for n in range(3):
            up_out(n).start()
        for n in range(4):
            own[n]().start()
            local[n]().start()
        for n in range(3):
            dn_out(n).start()
        for n in range(3):
            up_in(others[n]).wait_recv()
            pass_up(n).start()
        local[0]().wait()
        local[1]().wait()
        x_send().wait_recv()

    @pl.when(c == 1)
    def _():
        x_load(0).start()
        x_load(0).wait()
        x_send().start()
        for owner in range(4):
            up_in(owner).wait_recv()
        own[1]().wait_recv()

    merged_load(0, 0).wait()
    merge_up(0, 0)
    keep_rows(0)

    def tile_turn(r):
        merged_store(r, r % RING).start()

        @pl.when(r >= 1)
        def _():
            merged_store(r - 1, (r + 2) % RING).wait()

        @pl.when(r + 2 < 2 * nb)
        def _():
            base_loads(r + 2, (r + 2) % RING)

        @pl.when(r + 2 >= 2 * nb)
        def _():
            merged_load(r + 2 - 2 * nb, (r + 2) % RING).start()

        merged_load(0, (r + 1) % RING).wait()

    def first_up(r, carry):
        @pl.when(r == nb // 2)
        def _():
            @pl.when(c == 0)
            def _():
                for n in range(3):
                    dn_in(others[n]).wait_recv()
                    pass_dn(n).start()
        tile_turn(r)
        merge_up((r + 1) % RING, r + 1)
        dot_up(r % RING, r)
        return carry

    lax.fori_loop(0, nb - 1, first_up, 0)

    @pl.when(c == 0)
    def _():
        for n in range(3):
            up_out(n).wait_send()
            dn_out(n).wait_send()
            pass_up(n).wait_send()
            pass_dn(n).wait_send()
        for n in range(4):
            own[n]().wait_send()
        local[2]().wait()
        local[3]().wait()

    @pl.when(c == 1)
    def _():
        for owner in range(4):
            dn_in(owner).wait_recv()
        own[2]().wait_recv()

    tile_turn(nb - 1)
    merge_dn(nb % RING, 0)
    dot_up((nb - 1) % RING, nb - 1)

    def x_turn(k, r):
        @pl.when((k + 1 < nc) & (c == 0) & (r == nb))
        def _():
            pl.semaphore_signal(xfree, inc=1, device_id=(t, 1), device_id_type=MESH)

        @pl.when((k + 1 < nc) & (c == 1) & (r == nb))
        def _():
            @pl.when(k >= 0)
            def _():
                x_send().wait_send()
            x_load(k + 1).start()

        @pl.when((k + 1 < nc) & (c == 1) & (r == nb + 2))
        def _():
            x_load(k + 1).wait()
            pl.semaphore_wait(xfree, 1)
            x_send().start()

        @pl.when((k >= 1) & (r == 0))
        def _():
            @pl.when(c == 0)
            def _():
                x_send().wait_recv()
            keep_rows(k)

    def first_dn(r, carry):
        x_turn(0, r)
        tile_turn(r)
        merge_dn((r + 1) % RING, r + 1 - nb)
        dot_dn(r % RING, r % 2)
        swap(r - nb).start()
        stages(r)
        return carry

    lax.fori_loop(nb, 2 * nb - 1, first_dn, 0)

    def step(s, carry):
        k, r = s // (2 * nb), s % (2 * nb)
        x_turn(k, r)

        @pl.when(s == 2 * nb - 1)
        def _():
            tile_turn(2 * nb - 1)

        @pl.when(s == 2 * nb)
        def _():
            merged_store(2 * nb - 1, (2 * nb - 1) % RING).wait()

        @pl.when(s >= 2 * nb)
        def _():
            @pl.when(s + 2 < 2 * nb * nc)
            def _():
                merged_load((s + 2) % (2 * nb), (s + 2) % RING).start()

            @pl.when(s + 1 < 2 * nb * nc)
            def _():
                merged_load(0, (s + 1) % RING).wait()

        @pl.when(r < nb)
        def _():
            dot_up(s % RING, r)

        @pl.when(r >= nb)
        def _():
            dot_dn(s % RING, s % 2)
            swap(k * nb + r - nb).start()
        stages(s)
        return carry

    lax.fori_loop(2 * nb - 1, 2 * nb * nc, step, 0)

    def drain(s, carry):
        stages(s)
        return carry

    lax.fori_loop(2 * nb * nc, 2 * (total - 1) + nb + LAG[-1] + 1, drain, 0)

    @pl.when(c == 1)
    def _():
        x_send().wait_send()
        for n in range(3):
            part = hid.at[pl.ds(0, nc * mq), :]
            pltpu.make_async_copy(part, part, fsem.at[n]).wait()


def fused_mlp(base_up, base_down, a_up, b_up, a_dn, b_dn, prompts):
    tokens, d = prompts.shape[1:]
    fh = base_up.shape[2] // 2
    nb = fh // TILE
    w = d // nb
    m = min(CHUNK, tokens)
    nc = tokens // m
    rank = a_up.shape[1]
    dims = (m, nc, nb, d, fh, w)
    dma = pltpu.SemaphoreType.DMA
    anywhere = pl.BlockSpec(memory_space=pl.ANY)
    hid, _ = pl.pallas_call(
        functools.partial(mlp_kernel, dims),
        out_shape=(jax.ShapeDtypeStruct((tokens, d), BF16), jax.ShapeDtypeStruct((2 * nb, d, TILE), BF16)),
        in_specs=[anywhere] * 7,
        out_specs=(anywhere, anywhere),
        scratch_shapes=[
            pltpu.VMEM((m, d), BF16),
            pltpu.VMEM((m, fh), BF16),
            pltpu.VMEM((RING, d, TILE), BF16),
            pltpu.VMEM((d, rank), BF16),
            pltpu.VMEM((rank, fh), BF16),
            pltpu.VMEM((fh, rank), BF16),
            pltpu.VMEM((rank, d), BF16),
            pltpu.VMEM((2, m, w), F32),
            pltpu.VMEM((4, m // 2, w), F32),
            pltpu.VMEM((nb, m // 2, w), F32),
            pltpu.VMEM((nb, m // 4, w), F32),
            pltpu.VMEM((nb, m // 8, w), F32),
            pltpu.VMEM((nb, m // 4, w), BF16),
            pltpu.VMEM((2, m // 8, d), BF16),
            dma((RING,)), dma((RING,)), dma((4,)), dma((18,)), dma((10,)), dma((3,)),
            dma((2,)), dma((4,)), dma((nb,)), dma((nb,)), dma((nb,)), dma((nb,)), dma((nb,)), dma((nb,)),
            dma((nb,)), dma((nb,)), dma((3,)),
            pltpu.SemaphoreType.REGULAR, pltpu.SemaphoreType.REGULAR,
            pltpu.SemaphoreType.REGULAR, pltpu.SemaphoreType.REGULAR,
        ],
        compiler_params=pltpu.CompilerParams(has_side_effects=True, vmem_limit_bytes=67043328),
        name='mlp_ring',
    )(base_up, base_down, a_up, b_up, a_dn, b_dn, prompts)
    return hid


def solution(mesh):
    left_spec = P('pool', None, 'tp', None)
    right_spec = P('pool', None, None, 'tp')
    prompt_spec = P('pool', None, None)

    def local_step(base_up, base_down, up_left, up_right, down_left, down_right, grad_up_left, grad_up_right, grad_down_left, grad_down_right, learn_rate, prompts):
        step_size = learn_rate[0]
        new_up_left = up_left - step_size * grad_up_left
        new_up_right = up_right - step_size * grad_up_right
        new_down_left = down_left - step_size * grad_down_left
        new_down_right = down_right - step_size * grad_down_right
        own = tuple(part[0, 0].astype(BF16) for part in (new_up_left, new_up_right, new_down_left, new_down_right))
        hid = fused_mlp(base_up, base_down, *own, prompts)
        core = lax.axis_index('pool')
        hidden_out = jnp.where(core == 1, hid, jnp.zeros_like(hid))[None]
        return new_up_left, new_up_right, new_down_left, new_down_right, hidden_out

    return jax.shard_map(local_step, mesh=mesh,
                         in_specs=(P(None, None, 'tp'), P(None, 'tp', None), left_spec, right_spec, left_spec, right_spec, left_spec, right_spec, left_spec, right_spec, P(None), prompt_spec),
                         out_specs=(left_spec, right_spec, left_spec, right_spec, prompt_spec),
                         check_vma=False)
```

```python
import functools

import jax
import jax.numpy as jnp
from jax import lax
from jax.experimental import pallas as pl
from jax.experimental.pallas import tpu as pltpu
from jax.sharding import PartitionSpec as P

CHUNK = 256
TILE = 256
RING = 3
LAG = (4, 7, 9, 25)
BF16 = jnp.bfloat16
F32 = jnp.float32
MESH = pl.DeviceIdType.MESH


def mlp_kernel(dims, base_up, base_dn, a_up, a_up_g, b_up, b_up_g, a_dn, a_dn_g, b_dn, b_dn_g, rate, prompts, hid, wm,
               left, right, x, u, wb, aup, bup, adn, bdn, pb, rx0, s1, rx1, rx2, ob, res,
               wsem, osem, lsem, rsem, asend, arecv, xsem, s0, r0, ss1, rs1, ss2, rs2, ss3, rs3, ss4, ss5, fsem,
               xfree, cr1, cr2, cr3):
    m, nc, nb, d, fh, w = dims
    total = nc * nb
    ring = nb
    halves = w // TILE
    mh, mq, me = m // 2, m // 4, m // 8
    d4 = d // 4
    rank = aup.shape[1]
    t = lax.axis_index('tp')
    c = lax.axis_index('pool')
    xb, yb = t % 2, t // 2
    near_x, near_y = t + 1 - 2 * xb, t + 2 - 4 * yb
    b1 = (1 - c) * xb + c * yb
    b2 = c * xb + (1 - c) * yb
    p1 = (1 - c) * near_x + c * near_y
    p2 = c * near_x + (1 - c) * near_y

    def rows(start, size):
        return pl.ds(pl.multiple_of(start, size), size)

    def remote(src, dst, send, recv, device):
        return pltpu.make_async_remote_copy(src_ref=src, dst_ref=dst, send_sem=send, recv_sem=recv,
                                            device_id=device, device_id_type=MESH)

    def base_loads(r, slot):
        @pl.when(r < nb)
        def _():
            pltpu.make_async_copy(base_up.at[0, :, rows(c * fh + r * TILE, TILE)], wb.at[slot], wsem.at[slot]).start()

        @pl.when(r >= nb)
        def _():
            for h in range(halves):
                pltpu.make_async_copy(base_dn.at[0, rows(c * fh, fh), rows((r - nb) * w + h * TILE, TILE)],
                                      wb.at[slot, pl.ds(h * fh, fh), :], wsem.at[slot]).start()

    def merged_load(r, slot):
        return pltpu.make_async_copy(wm.at[r], wb.at[slot], wsem.at[slot])

    def merged_store(r, slot):
        return pltpu.make_async_copy(wb.at[slot], wm.at[r], osem.at[slot])

    piece = min(512, fh)

    def merge_up(slot, j):
        right = bup[:, rows(j * TILE, TILE)]
        for q in range(d // piece):
            part = pl.ds(q * piece, piece)
            delta = jnp.dot(aup[part, :], right, preferred_element_type=F32).astype(BF16)
            wb[slot, part, :] = wb[slot, part, :] + delta

    def merge_dn(slot, i):
        for h in range(halves):
            right = bdn[:, rows(i * w + h * TILE, TILE)]
            for q in range(fh // piece):
                delta = jnp.dot(adn[pl.ds(q * piece, piece), :], right, preferred_element_type=F32).astype(BF16)
                part = pl.ds(h * fh + q * piece, piece)
                wb[slot, part, :] = wb[slot, part, :] + delta

    def dot_up(slot, j):
        pre = jnp.dot(x[...], wb[slot], preferred_element_type=F32)
        u[:, rows(j * TILE, TILE)] = jax.nn.gelu(pre, approximate=True).astype(BF16)

    def dot_dn(slot, buf):
        for h in range(halves):
            pb[buf, :, pl.ds(h * TILE, TILE)] = jnp.dot(u[...], wb[slot, pl.ds(h * fh, fh), :],
                                                        preferred_element_type=F32)

    def swap(g):
        return remote(pb.at[g % 2, rows((1 - c) * mh, mh), :], rx0.at[g % 4], s0.at[g % 2], r0.at[g % 4], (t, 1 - c))

    def first(g):
        return remote(s1.at[g % ring, rows((1 - b1) * mq, mq), :], rx1.at[g % ring],
                      ss1.at[g % ring], rs1.at[g % ring], (p1, c))

    def second(g):
        return remote(s1.at[g % ring, rows(b1 * mq + (1 - b2) * me, me), :], rx2.at[g % ring],
                      ss2.at[g % ring], rs2.at[g % ring], (p2, c))

    def gather(g):
        half = ob.at[g % ring, rows(b2 * me, me), :]
        return remote(half, half, ss3.at[g % ring], rs3.at[g % ring], (p2, c))

    def final_place(g):
        return hid.at[rows((g // nb) * m + c * mh + b1 * mq, mq), rows((g % nb) * w, w)]

    def final_far(g):
        return remote(ob.at[g % ring], final_place(g), ss4.at[g % ring], fsem.at[1 + c], (p1, 1))

    def final_near(g):
        return remote(ob.at[g % ring], final_place(g), ss5.at[g % ring], fsem.at[0], (t, 1))

    def final_local(g):
        return pltpu.make_async_copy(ob.at[g % ring], final_place(g), ss5.at[g % ring])

    def stage_a(g):
        slot = g % ring
        swap(g).wait_send()
        swap(g).wait_recv()
        s1[slot] = pb[g % 2, rows(c * mh, mh), :] + rx0[g % 4]

        @pl.when(g >= ring)
        def _():
            pl.semaphore_wait(cr1, 1)
        first(g).start()

    def stage_b(g):
        slot = g % ring
        keep = rows(b1 * mq, mq)
        first(g).wait_recv()
        s1[slot, keep, :] = s1[slot, keep, :] + rx1[slot]

        @pl.when(g + ring < total)
        def _():
            pl.semaphore_signal(cr1, inc=1, device_id=(p1, c), device_id_type=MESH)

        @pl.when(g >= ring)
        def _():
            pl.semaphore_wait(cr2, 1)
        second(g).start()

    def stage_c(g):
        slot = g % ring
        keep = rows(b1 * mq + b2 * me, me)
        second(g).wait_recv()
        first(g).wait_send()
        held = res[(g // nb) % 2, :, rows((g % nb) * w, w)].astype(F32)
        ob[slot, rows(b2 * me, me), :] = (held + (s1[slot, keep, :] + rx2[slot])).astype(BF16)

        @pl.when(g + ring < total)
        def _():
            pl.semaphore_signal(cr2, inc=1, device_id=(p2, c), device_id_type=MESH)

        @pl.when(g >= ring)
        def _():
            pl.semaphore_wait(cr3, 1)
        gather(g).start()

    def stage_d(g):
        gather(g).wait_recv()
        second(g).wait_send()
        final_far(g).start()

        @pl.when(c == 0)
        def _():
            final_near(g).start()

        @pl.when(c == 1)
        def _():
            final_local(g).start()

    def stage_e(g):
        gather(g).wait_send()
        final_far(g).wait_send()

        @pl.when(c == 0)
        def _():
            final_near(g).wait_send()

        @pl.when(c == 1)
        def _():
            final_local(g).wait()

        @pl.when(g + ring < total)
        def _():
            pl.semaphore_signal(cr3, inc=1, device_id=(p2, c), device_id_type=MESH)

    def stages(s):
        before = s - 1
        r = before % (2 * nb)

        @pl.when((r >= nb) & (before < 2 * nb * nc))
        def _():
            stage_a((before // (2 * nb)) * nb + r - nb)
        for lag, stage in zip(LAG, (stage_b, stage_c, stage_d, stage_e)):
            late = s - nb - lag

            @pl.when((late >= 0) & (late % 2 == 0) & (late < 2 * total))
            def _():
                stage(late // 2)

    def x_load(k):
        return pltpu.make_async_copy(prompts.at[0, rows(k * m, m), :], x, xsem.at[0])

    def x_send():
        return remote(x, x, xsem.at[1], xsem.at[2], (t, 0))

    def keep_rows(k):
        res[k % 2] = x[rows(c * mh + b1 * mq + b2 * me, me), :]

    def up_piece(owner):
        return aup.at[rows(owner * d4, d4), :]

    def dn_piece(owner):
        return bdn.at[:, rows(owner * d4, d4)]

    others = (near_x, near_y, 3 - t)

    def up_out(n):
        return remote(up_piece(t), up_piece(t), asend.at[n], arecv.at[t], (others[n], 0))

    def dn_out(n):
        return remote(dn_piece(t), dn_piece(t), asend.at[3 + n], arecv.at[4 + t], (others[n], 0))

    def up_in(owner):
        return remote(up_piece(owner), up_piece(owner), asend.at[6], arecv.at[owner], (t, 1))

    def dn_in(owner):
        return remote(dn_piece(owner), dn_piece(owner), asend.at[7], arecv.at[4 + owner], (t, 1))

    def pass_up(n):
        return remote(up_piece(others[n]), up_piece(others[n]), asend.at[8 + n], arecv.at[others[n]], (t, 1))

    def pass_dn(n):
        return remote(dn_piece(others[n]), dn_piece(others[n]), asend.at[11 + n], arecv.at[4 + others[n]], (t, 1))

    far_b = u.at[pl.ds(0, rank), :]
    far_a = wb.at[2, pl.ds(0, fh), pl.ds(0, rank)]
    own = (
        lambda: remote(up_piece(t), up_piece(t), asend.at[14], arecv.at[t], (t, 1)),
        lambda: remote(far_b, bup, asend.at[15], arecv.at[8], (t, 1)),
        lambda: remote(far_a, adn, asend.at[16], arecv.at[9], (t, 1)),
        lambda: remote(dn_piece(t), dn_piece(t), asend.at[17], arecv.at[4 + t], (t, 1)),
    )

    size = d4 // 2
    lefts = [(a_up, a_up_g, q, aup, t * d4 + q * size) for q in range(2)]
    lefts += [(a_dn, a_dn_g, q, adn, q * size) for q in range(4)]
    lefts += [(a_dn, a_dn_g, 4 + q, None, q * size) for q in range(4)]
    rights = [(b_up, b_up_g, q, bup, q * size) for q in range(4)]
    rights += [(b_up, b_up_g, 4 + q, u, q * size) for q in range(4)]
    rights += [(b_dn, b_dn_g, q, bdn, t * d4 + q * size) for q in range(2)]

    def left_load(n):
        value, grad, q, _, _ = lefts[n]
        for side, src in enumerate((value, grad)):
            pltpu.make_async_copy(src.at[0, 0, pl.ds(q * size, size), :], left.at[n % 2, side], lsem.at[n % 2]).start()

    def right_load(n):
        value, grad, q, _, _ = rights[n]
        for side, src in enumerate((value, grad)):
            pltpu.make_async_copy(src.at[0, 0, :, pl.ds(q * size, size)], right.at[n % 2, side], rsem.at[n % 2]).start()

    def left_update(n):
        _, _, _, dst, start = lefts[n]
        pltpu.make_async_copy(left.at[n % 2], left.at[n % 2], lsem.at[n % 2]).wait()
        new = (left[n % 2, 0] - rate[0] * left[n % 2, 1]).astype(BF16)
        if dst is None:
            wb[2, rows(start, size), pl.ds(0, rank)] = new
        else:
            dst[rows(start, size), :] = new
        if n + 2 < len(lefts):
            left_load(n + 2)

    def right_update(n):
        _, _, _, dst, start = rights[n]
        pltpu.make_async_copy(right.at[n % 2], right.at[n % 2], rsem.at[n % 2]).wait()
        new = (right[n % 2, 0] - rate[0] * right[n % 2, 1]).astype(BF16)
        if dst is u:
            u[pl.ds(0, rank), rows(start, size)] = new
        else:
            dst[:, rows(start, size)] = new
        if n + 2 < len(rights):
            right_load(n + 2)

    @pl.when(c == 0)
    def _():
        for n in range(2):
            left_load(n)
        for n in range(2):
            right_load(n)
        base_loads(0, 0)
        base_loads(1, 1)
        for n in range(2):
            left_update(n)
        for n in range(3):
            up_out(n).start()
        own[0]().start()
        for n in range(8):
            right_update(n)
        own[1]().start()
        for n in range(8, 10):
            right_update(n)
        for n in range(3):
            dn_out(n).start()
        own[3]().start()
        for n in range(2, 10):
            left_update(n)
        own[2]().start()
        for n in range(3):
            up_in(others[n]).wait_recv()
            pass_up(n).start()
        own[1]().wait_send()
        own[2]().wait_send()
        x_send().wait_recv()

    @pl.when(c == 1)
    def _():
        x_load(0).start()
        base_loads(0, 0)
        base_loads(1, 1)
        x_load(0).wait()
        x_send().start()
        for owner in range(4):
            up_in(owner).wait_recv()
        own[1]().wait_recv()

    merged_load(0, 0).wait()
    merge_up(0, 0)
    keep_rows(0)

    def tile_turn(r):
        merged_store(r, r % RING).start()

        @pl.when(r >= 1)
        def _():
            merged_store(r - 1, (r + 2) % RING).wait()

        @pl.when(r + 2 < 2 * nb)
        def _():
            base_loads(r + 2, (r + 2) % RING)

        @pl.when(r + 2 >= 2 * nb)
        def _():
            merged_load(r + 2 - 2 * nb, (r + 2) % RING).start()

        merged_load(0, (r + 1) % RING).wait()

    def first_up(r, carry):
        @pl.when(r == nb // 2)
        def _():
            @pl.when(c == 0)
            def _():
                for n in range(3):
                    dn_in(others[n]).wait_recv()
                    pass_dn(n).start()
        tile_turn(r)
        dot_up(r % RING, r)

        @pl.when(r < nb)
        def _():
            merge_up((r + 1) % RING, r + 1)
        return carry

    lax.fori_loop(0, nb - 1, first_up, 0)

    @pl.when(c == 0)
    def _():
        for n in range(3):
            up_out(n).wait_send()
            dn_out(n).wait_send()
            pass_up(n).wait_send()
            pass_dn(n).wait_send()
        own[0]().wait_send()
        own[3]().wait_send()

    @pl.when(c == 1)
    def _():
        for owner in range(4):
            dn_in(owner).wait_recv()
        own[2]().wait_recv()

    tile_turn(nb - 1)
    merge_dn(nb % RING, 0)
    dot_up((nb - 1) % RING, nb - 1)

    def x_turn(k, r):
        @pl.when((k + 1 < nc) & (c == 0) & (r == nb))
        def _():
            pl.semaphore_signal(xfree, inc=1, device_id=(t, 1), device_id_type=MESH)

        @pl.when((k + 1 < nc) & (c == 1) & (r == nb))
        def _():
            @pl.when(k >= 0)
            def _():
                x_send().wait_send()
            x_load(k + 1).start()

        @pl.when((k + 1 < nc) & (c == 1) & (r == nb + 2))
        def _():
            x_load(k + 1).wait()
            pl.semaphore_wait(xfree, 1)
            x_send().start()

        @pl.when((k >= 1) & (r == 0))
        def _():
            @pl.when(c == 0)
            def _():
                x_send().wait_recv()
            keep_rows(k)

    def first_dn(r, carry):
        x_turn(0, r)
        tile_turn(r)
        dot_dn(r % RING, r % 2)
        merge_dn((r + 1) % RING, r + 1 - nb)
        swap(r - nb).start()
        stages(r)
        return carry

    lax.fori_loop(nb, 2 * nb - 1, first_dn, 0)

    def step(s, carry):
        k, r = s // (2 * nb), s % (2 * nb)
        x_turn(k, r)

        @pl.when(s == 2 * nb - 1)
        def _():
            tile_turn(2 * nb - 1)

        @pl.when(s == 2 * nb)
        def _():
            merged_store(2 * nb - 1, (2 * nb - 1) % RING).wait()

        @pl.when(s >= 2 * nb)
        def _():
            @pl.when(s + 2 < 2 * nb * nc)
            def _():
                merged_load((s + 2) % (2 * nb), (s + 2) % RING).start()

            @pl.when(s + 1 < 2 * nb * nc)
            def _():
                merged_load(0, (s + 1) % RING).wait()

        @pl.when(r < nb)
        def _():
            dot_up(s % RING, r)

        @pl.when(r >= nb)
        def _():
            dot_dn(s % RING, s % 2)
            swap(k * nb + r - nb).start()
        stages(s)
        return carry

    lax.fori_loop(2 * nb - 1, 2 * nb * nc, step, 0)

    def drain(s, carry):
        stages(s)
        return carry

    lax.fori_loop(2 * nb * nc, 2 * (total - 1) + nb + LAG[-1] + 1, drain, 0)

    @pl.when(c == 1)
    def _():
        x_send().wait_send()
        for n in range(3):
            part = hid.at[pl.ds(0, nc * mq), :]
            pltpu.make_async_copy(part, part, fsem.at[n]).wait()


def fused_mlp(base_up, base_down, factors, learn_rate, prompts):
    tokens, d = prompts.shape[1:]
    fh = base_up.shape[2] // 2
    nb = fh // TILE
    w = d // nb
    m = min(CHUNK, tokens)
    nc = tokens // m
    rank = factors[0].shape[3]
    dims = (m, nc, nb, d, fh, w)
    dma = pltpu.SemaphoreType.DMA
    anywhere = pl.BlockSpec(memory_space=pl.ANY)
    hid, _ = pl.pallas_call(
        functools.partial(mlp_kernel, dims),
        out_shape=(jax.ShapeDtypeStruct((tokens, d), BF16), jax.ShapeDtypeStruct((2 * nb, d, TILE), BF16)),
        in_specs=[anywhere] * 10 + [pl.BlockSpec(memory_space=pltpu.SMEM), anywhere],
        out_specs=(anywhere, anywhere),
        scratch_shapes=[
            pltpu.VMEM((2, 2, d // 8, rank), F32),
            pltpu.VMEM((2, 2, rank, d // 8), F32),
            pltpu.VMEM((m, d), BF16),
            pltpu.VMEM((m, fh), BF16),
            pltpu.VMEM((RING, d, TILE), BF16),
            pltpu.VMEM((d, rank), BF16),
            pltpu.VMEM((rank, fh), BF16),
            pltpu.VMEM((fh, rank), BF16),
            pltpu.VMEM((rank, d), BF16),
            pltpu.VMEM((2, m, w), F32),
            pltpu.VMEM((4, m // 2, w), F32),
            pltpu.VMEM((nb, m // 2, w), F32),
            pltpu.VMEM((nb, m // 4, w), F32),
            pltpu.VMEM((nb, m // 8, w), F32),
            pltpu.VMEM((nb, m // 4, w), BF16),
            pltpu.VMEM((2, m // 8, d), BF16),
            dma((RING,)), dma((RING,)), dma((2,)), dma((2,)), dma((18,)), dma((10,)), dma((3,)),
            dma((2,)), dma((4,)), dma((nb,)), dma((nb,)), dma((nb,)), dma((nb,)), dma((nb,)), dma((nb,)),
            dma((nb,)), dma((nb,)), dma((3,)),
            pltpu.SemaphoreType.REGULAR, pltpu.SemaphoreType.REGULAR,
            pltpu.SemaphoreType.REGULAR, pltpu.SemaphoreType.REGULAR,
        ],
        compiler_params=pltpu.CompilerParams(has_side_effects=True, vmem_limit_bytes=67043328),
        name='mlp_ring',
    )(base_up, base_down, *factors, learn_rate, prompts)
    return hid


def solution(mesh):
    left_spec = P('pool', None, 'tp', None)
    right_spec = P('pool', None, None, 'tp')
    prompt_spec = P('pool', None, None)

    def local_step(base_up, base_down, up_left, up_right, down_left, down_right, grad_up_left, grad_up_right, grad_down_left, grad_down_right, learn_rate, prompts):
        step_size = learn_rate[0]
        new_up_left = up_left - step_size * grad_up_left
        new_up_right = up_right - step_size * grad_up_right
        new_down_left = down_left - step_size * grad_down_left
        new_down_right = down_right - step_size * grad_down_right
        factors = (up_left, grad_up_left, up_right, grad_up_right, down_left, grad_down_left, down_right, grad_down_right)
        hid = fused_mlp(base_up, base_down, factors, learn_rate, prompts)
        core = lax.axis_index('pool')
        hidden_out = jnp.where(core == 1, hid, jnp.zeros_like(hid))[None]
        return new_up_left, new_up_right, new_down_left, new_down_right, hidden_out

    return jax.shard_map(local_step, mesh=mesh,
                         in_specs=(P(None, None, 'tp'), P(None, 'tp', None), left_spec, right_spec, left_spec, right_spec, left_spec, right_spec, left_spec, right_spec, P(None), prompt_spec),
                         out_specs=(left_spec, right_spec, left_spec, right_spec, prompt_spec),
                         check_vma=False)
```

```python
import functools

import jax
import jax.numpy as jnp
from jax import lax
from jax.experimental import pallas as pl
from jax.experimental.pallas import tpu as pltpu
from jax.sharding import PartitionSpec as P

CHUNK = 512
TILE = 256
RING = 3
LAG = (2, 4, 7, 23)
BF16 = jnp.bfloat16
F32 = jnp.float32
MESH = pl.DeviceIdType.MESH


def mlp_kernel(dims, base_up, base_dn, a_up, a_up_g, b_up, b_up_g, a_dn, a_dn_g, b_dn, b_dn_g, rate, prompts, hid, tail, near, wm,
               left, right, x, u, wb, aup, bup, adn, bdn, pb, rx0, s1, rx1, rx2, ob, res,
               wsem, osem, lsem, rsem, asend, arecv, xsem, s0, r0, ss1, rs1, ss2, rs2, ss3, rs3, ss4, ss5, fsem,
               xfree, cr1, cr2, cr3):
    m, nc, nb, d, fh, w = dims
    total = nc * nb
    ring = nb
    halves = w // TILE
    mh, mq, me = m // 2, m // 4, m // 8
    d4 = d // 4
    rank = aup.shape[1]
    t = lax.axis_index('tp')
    c = lax.axis_index('pool')
    xb, yb = t % 2, t // 2
    near_x, near_y = t + 1 - 2 * xb, t + 2 - 4 * yb
    b1 = (1 - c) * xb + c * yb
    b2 = c * xb + (1 - c) * yb
    p1 = (1 - c) * near_x + c * near_y
    p2 = c * near_x + (1 - c) * near_y

    def rows(start, size):
        return pl.ds(pl.multiple_of(start, size), size)

    def remote(src, dst, send, recv, device):
        return pltpu.make_async_remote_copy(src_ref=src, dst_ref=dst, send_sem=send, recv_sem=recv,
                                            device_id=device, device_id_type=MESH)

    def base_loads(r, slot):
        @pl.when(r < nb)
        def _():
            pltpu.make_async_copy(base_up.at[0, :, rows(c * fh + r * TILE, TILE)], wb.at[slot], wsem.at[slot]).start()

        @pl.when(r >= nb)
        def _():
            for h in range(halves):
                pltpu.make_async_copy(base_dn.at[0, rows(c * fh, fh), rows((r - nb) * w + h * TILE, TILE)],
                                      wb.at[slot, pl.ds(h * fh, fh), :], wsem.at[slot]).start()

    def merged_load(r, slot):
        return pltpu.make_async_copy(wm.at[r], wb.at[slot], wsem.at[slot])

    def merged_store(r, slot):
        return pltpu.make_async_copy(wb.at[slot], wm.at[r], osem.at[slot])

    piece = min(512, fh)

    def merge_up(slot, j):
        right = bup[:, rows(j * TILE, TILE)]
        for q in range(d // piece):
            part = pl.ds(q * piece, piece)
            delta = jnp.dot(aup[part, :], right, preferred_element_type=F32).astype(BF16)
            wb[slot, part, :] = wb[slot, part, :] + delta

    def merge_dn(slot, i):
        for h in range(halves):
            right = bdn[:, rows(i * w + h * TILE, TILE)]
            for q in range(fh // piece):
                delta = jnp.dot(adn[pl.ds(q * piece, piece), :], right, preferred_element_type=F32).astype(BF16)
                part = pl.ds(h * fh + q * piece, piece)
                wb[slot, part, :] = wb[slot, part, :] + delta

    def dot_up(slot, j):
        pre = jnp.dot(x[...], wb[slot], preferred_element_type=F32)
        u[:, rows(j * TILE, TILE)] = jax.nn.gelu(pre, approximate=True).astype(BF16)

    def dot_dn(slot, buf):
        for h in range(halves):
            pb[buf, :, pl.ds(h * TILE, TILE)] = jnp.dot(u[...], wb[slot, pl.ds(h * fh, fh), :],
                                                        preferred_element_type=F32)

    def swap(g):
        return remote(pb.at[g % 2, rows((1 - c) * mh, mh), :], rx0.at[g % 4], s0.at[g % 2], r0.at[g % 4], (t, 1 - c))

    def first(g):
        return remote(s1.at[g % ring, rows((1 - b1) * mq, mq), :], rx1.at[g % ring],
                      ss1.at[g % ring], rs1.at[g % ring], (p1, c))

    def second(g):
        return remote(s1.at[g % ring, rows(b1 * mq + (1 - b2) * me, me), :], rx2.at[g % ring],
                      ss2.at[g % ring], rs2.at[g % ring], (p2, c))

    def gather(g):
        half = ob.at[g % ring, rows(b2 * me, me), :]
        return remote(half, half, ss3.at[g % ring], rs3.at[g % ring], (p2, c))

    def final_place(g):
        return hid.at[rows((g // nb) * m + c * mh + b1 * mq, mq), rows((g % nb) * w, w)]

    def final_far(g):
        return remote(ob.at[g % ring], final_place(g), ss4.at[g % ring], fsem.at[1 + c], (p1, 1))

    def final_near(g):
        return remote(ob.at[g % ring], final_place(g), ss5.at[g % ring], fsem.at[0], (t, 1))

    def final_local(g):
        return pltpu.make_async_copy(ob.at[g % ring], final_place(g), ss5.at[g % ring])

    def stage_a(g):
        slot = g % ring
        swap(g).wait_send()
        swap(g).wait_recv()
        s1[slot] = pb[g % 2, rows(c * mh, mh), :] + rx0[g % 4]

        @pl.when(g >= ring)
        def _():
            pl.semaphore_wait(cr1, 1)
        first(g).start()

    def stage_b(g):
        slot = g % ring
        keep = rows(b1 * mq, mq)
        first(g).wait_recv()
        s1[slot, keep, :] = s1[slot, keep, :] + rx1[slot]

        @pl.when(g + ring < total)
        def _():
            pl.semaphore_signal(cr1, inc=1, device_id=(p1, c), device_id_type=MESH)

        @pl.when(g >= ring)
        def _():
            pl.semaphore_wait(cr2, 1)
        second(g).start()

    def stage_c(g):
        slot = g % ring
        keep = rows(b1 * mq + b2 * me, me)
        second(g).wait_recv()
        first(g).wait_send()
        held = res[(g // nb) % 2, :, rows((g % nb) * w, w)].astype(F32)
        ob[slot, rows(b2 * me, me), :] = (held + (s1[slot, keep, :] + rx2[slot])).astype(BF16)

        @pl.when(g + ring < total)
        def _():
            pl.semaphore_signal(cr2, inc=1, device_id=(p2, c), device_id_type=MESH)

        @pl.when(g >= ring)
        def _():
            pl.semaphore_wait(cr3, 1)
        gather(g).start()

    def tail_local(g):
        return pltpu.make_async_copy(ob.at[g % ring], tail.at[:, rows((g % nb) * w, w)], ss4.at[g % ring])

    def tail_near(g):
        return remote(ob.at[g % ring], near.at[:, rows((g % nb) * w, w)], ss5.at[g % ring], fsem.at[3], (t, 1))

    def stage_d(g):
        gather(g).wait_recv()
        second(g).wait_send()

        @pl.when(g < total - nb)
        def _():
            final_far(g).start()

            @pl.when(c == 0)
            def _():
                final_near(g).start()

            @pl.when(c == 1)
            def _():
                final_local(g).start()

        @pl.when(g >= total - nb)
        def _():
            tail_local(g).start()

            @pl.when(c == 0)
            def _():
                tail_near(g).start()

    def stage_e(g):
        gather(g).wait_send()

        @pl.when(g < total - nb)
        def _():
            final_far(g).wait_send()

            @pl.when(c == 0)
            def _():
                final_near(g).wait_send()

            @pl.when(c == 1)
            def _():
                final_local(g).wait()

        @pl.when(g >= total - nb)
        def _():
            tail_local(g).wait()

            @pl.when(c == 0)
            def _():
                tail_near(g).wait_send()

        @pl.when(g + ring < total)
        def _():
            pl.semaphore_signal(cr3, inc=1, device_id=(p2, c), device_id_type=MESH)

    def stages(s):
        before = s - 1
        r = before % (2 * nb)

        @pl.when((r >= nb) & (before < 2 * nb * nc))
        def _():
            stage_a((before // (2 * nb)) * nb + r - nb)
        for lag, stage in zip(LAG, (stage_b, stage_c, stage_d, stage_e)):
            late = s - nb - lag

            @pl.when((late >= 0) & (late % 2 == 0) & (late < 2 * total))
            def _():
                stage(late // 2)

    def x_load(k):
        return pltpu.make_async_copy(prompts.at[0, rows(k * m, m), :], x, xsem.at[0])

    def x_send():
        return remote(x, x, xsem.at[1], xsem.at[2], (t, 0))

    def keep_rows(k):
        res[k % 2] = x[rows(c * mh + b1 * mq + b2 * me, me), :]

    def up_piece(owner):
        return aup.at[rows(owner * d4, d4), :]

    def dn_piece(owner):
        return bdn.at[:, rows(owner * d4, d4)]

    others = (near_x, near_y, 3 - t)

    def up_out(n):
        return remote(up_piece(t), up_piece(t), asend.at[n], arecv.at[t], (others[n], 0))

    def dn_out(n):
        return remote(dn_piece(t), dn_piece(t), asend.at[3 + n], arecv.at[4 + t], (others[n], 0))

    def up_in(owner):
        return remote(up_piece(owner), up_piece(owner), asend.at[6], arecv.at[owner], (t, 1))

    def dn_in(owner):
        return remote(dn_piece(owner), dn_piece(owner), asend.at[7], arecv.at[4 + owner], (t, 1))

    def pass_up(n):
        return remote(up_piece(others[n]), up_piece(others[n]), asend.at[8 + n], arecv.at[others[n]], (t, 1))

    def pass_dn(n):
        return remote(dn_piece(others[n]), dn_piece(others[n]), asend.at[11 + n], arecv.at[4 + others[n]], (t, 1))

    far_b = u.at[pl.ds(0, rank), :]
    far_a = wb.at[2, pl.ds(0, fh), pl.ds(0, rank)]
    own = (
        lambda: remote(up_piece(t), up_piece(t), asend.at[14], arecv.at[t], (t, 1)),
        lambda: remote(far_b, bup, asend.at[15], arecv.at[8], (t, 1)),
        lambda: remote(far_a, adn, asend.at[16], arecv.at[9], (t, 1)),
        lambda: remote(dn_piece(t), dn_piece(t), asend.at[17], arecv.at[4 + t], (t, 1)),
    )

    size = d4 // 2
    lefts = [(a_up, a_up_g, q, aup, t * d4 + q * size) for q in range(2)]
    lefts += [(a_dn, a_dn_g, q, adn, q * size) for q in range(4)]
    lefts += [(a_dn, a_dn_g, 4 + q, None, q * size) for q in range(4)]
    rights = [(b_up, b_up_g, q, bup, q * size) for q in range(4)]
    rights += [(b_up, b_up_g, 4 + q, u, q * size) for q in range(4)]
    rights += [(b_dn, b_dn_g, q, bdn, t * d4 + q * size) for q in range(2)]

    def left_load(n):
        value, grad, q, _, _ = lefts[n]
        for side, src in enumerate((value, grad)):
            pltpu.make_async_copy(src.at[0, 0, pl.ds(q * size, size), :], left.at[n % 2, side], lsem.at[n % 2]).start()

    def right_load(n):
        value, grad, q, _, _ = rights[n]
        for side, src in enumerate((value, grad)):
            pltpu.make_async_copy(src.at[0, 0, :, pl.ds(q * size, size)], right.at[n % 2, side], rsem.at[n % 2]).start()

    def left_update(n):
        _, _, _, dst, start = lefts[n]
        pltpu.make_async_copy(left.at[n % 2], left.at[n % 2], lsem.at[n % 2]).wait()
        new = (left[n % 2, 0] - rate[0] * left[n % 2, 1]).astype(BF16)
        if dst is None:
            wb[2, rows(start, size), pl.ds(0, rank)] = new
        else:
            dst[rows(start, size), :] = new
        if n + 2 < len(lefts):
            left_load(n + 2)

    def right_update(n):
        _, _, _, dst, start = rights[n]
        pltpu.make_async_copy(right.at[n % 2], right.at[n % 2], rsem.at[n % 2]).wait()
        new = (right[n % 2, 0] - rate[0] * right[n % 2, 1]).astype(BF16)
        if dst is u:
            u[pl.ds(0, rank), rows(start, size)] = new
        else:
            dst[:, rows(start, size)] = new
        if n + 2 < len(rights):
            right_load(n + 2)

    @pl.when(c == 0)
    def _():
        for n in range(2):
            left_load(n)
        for n in range(2):
            right_load(n)
        base_loads(0, 0)
        base_loads(1, 1)
        for n in range(2):
            left_update(n)
        for n in range(3):
            up_out(n).start()
        own[0]().start()
        for n in range(8):
            right_update(n)
        own[1]().start()
        for n in range(8, 10):
            right_update(n)
        for n in range(3):
            dn_out(n).start()
        own[3]().start()
        for n in range(2, 10):
            left_update(n)
        own[2]().start()
        for n in range(3):
            up_in(others[n]).wait_recv()
            pass_up(n).start()
        own[1]().wait_send()
        own[2]().wait_send()
        x_send().wait_recv()

    @pl.when(c == 1)
    def _():
        x_load(0).start()
        base_loads(0, 0)
        base_loads(1, 1)
        x_load(0).wait()
        x_send().start()
        for owner in range(4):
            up_in(owner).wait_recv()
        own[1]().wait_recv()

    merged_load(0, 0).wait()
    merge_up(0, 0)
    keep_rows(0)

    def tile_turn(r):
        merged_store(r, r % RING).start()

        @pl.when(r >= 1)
        def _():
            merged_store(r - 1, (r + 2) % RING).wait()

        @pl.when(r + 2 < 2 * nb)
        def _():
            base_loads(r + 2, (r + 2) % RING)

        @pl.when(r + 2 >= 2 * nb)
        def _():
            merged_load(r + 2 - 2 * nb, (r + 2) % RING).start()

        merged_load(0, (r + 1) % RING).wait()

    def first_up(r, carry):
        @pl.when(r == nb // 2)
        def _():
            @pl.when(c == 0)
            def _():
                for n in range(3):
                    dn_in(others[n]).wait_recv()
                    pass_dn(n).start()
        tile_turn(r)
        dot_up(r % RING, r)

        @pl.when(r < nb)
        def _():
            merge_up((r + 1) % RING, r + 1)
        return carry

    lax.fori_loop(0, nb - 1, first_up, 0)

    @pl.when(c == 0)
    def _():
        for n in range(3):
            up_out(n).wait_send()
            dn_out(n).wait_send()
            pass_up(n).wait_send()
            pass_dn(n).wait_send()
        own[0]().wait_send()
        own[3]().wait_send()

    @pl.when(c == 1)
    def _():
        for owner in range(4):
            dn_in(owner).wait_recv()
        own[2]().wait_recv()

    tile_turn(nb - 1)
    merge_dn(nb % RING, 0)
    dot_up((nb - 1) % RING, nb - 1)

    def x_turn(k, r):
        @pl.when((k + 1 < nc) & (c == 0) & (r == nb))
        def _():
            pl.semaphore_signal(xfree, inc=1, device_id=(t, 1), device_id_type=MESH)

        @pl.when((k + 1 < nc) & (c == 1) & (r == nb))
        def _():
            @pl.when(k >= 0)
            def _():
                x_send().wait_send()
            x_load(k + 1).start()

        @pl.when((k + 1 < nc) & (c == 1) & (r == nb + 2))
        def _():
            x_load(k + 1).wait()
            pl.semaphore_wait(xfree, 1)
            x_send().start()

        @pl.when((k >= 1) & (r == 0))
        def _():
            @pl.when(c == 0)
            def _():
                x_send().wait_recv()
            keep_rows(k)

    def first_dn(r, carry):
        x_turn(0, r)
        tile_turn(r)
        dot_dn(r % RING, r % 2)
        merge_dn((r + 1) % RING, r + 1 - nb)
        swap(r - nb).start()
        stages(r)
        return carry

    lax.fori_loop(nb, 2 * nb - 1, first_dn, 0)

    def step(s, carry):
        k, r = s // (2 * nb), s % (2 * nb)
        x_turn(k, r)

        @pl.when(s == 2 * nb - 1)
        def _():
            tile_turn(2 * nb - 1)

        @pl.when(s == 2 * nb)
        def _():
            merged_store(2 * nb - 1, (2 * nb - 1) % RING).wait()

        @pl.when(s >= 2 * nb)
        def _():
            @pl.when(s + 2 < 2 * nb * nc)
            def _():
                merged_load((s + 2) % (2 * nb), (s + 2) % RING).start()

            @pl.when(s > 2 * nb)
            def _():
                merged_load(0, s % RING).wait()

        @pl.when(r < nb)
        def _():
            dot_up(s % RING, r)

        @pl.when(r >= nb)
        def _():
            dot_dn(s % RING, s % 2)
            swap(k * nb + r - nb).start()
        stages(s)
        return carry

    lax.fori_loop(2 * nb - 1, 2 * nb * nc, step, 0)

    def drain(s, carry):
        stages(s)
        return carry

    lax.fori_loop(2 * nb * nc, 2 * (total - 1) + nb + LAG[-1] + 1, drain, 0)

    @pl.when(c == 1)
    def _():
        x_send().wait_send()
        for n in range(3):
            part = hid.at[pl.ds(0, (nc - 1) * mq), :]
            pltpu.make_async_copy(part, part, fsem.at[n]).wait()
        pltpu.make_async_copy(near, near, fsem.at[3]).wait()


def fused_mlp(base_up, base_down, factors, learn_rate, prompts):
    tokens, d = prompts.shape[1:]
    fh = base_up.shape[2] // 2
    nb = fh // TILE
    w = d // nb
    m = min(CHUNK, tokens)
    nc = tokens // m
    rank = factors[0].shape[3]
    dims = (m, nc, nb, d, fh, w)
    dma = pltpu.SemaphoreType.DMA
    anywhere = pl.BlockSpec(memory_space=pl.ANY)
    hid, tail, near, _ = pl.pallas_call(
        functools.partial(mlp_kernel, dims),
        out_shape=(jax.ShapeDtypeStruct((tokens, d), BF16), jax.ShapeDtypeStruct((m // 4, d), BF16),
                   jax.ShapeDtypeStruct((m // 4, d), BF16), jax.ShapeDtypeStruct((2 * nb, d, TILE), BF16)),
        in_specs=[anywhere] * 10 + [pl.BlockSpec(memory_space=pltpu.SMEM), anywhere],
        out_specs=(anywhere,) * 4,
        scratch_shapes=[
            pltpu.VMEM((2, 2, d // 8, rank), F32),
            pltpu.VMEM((2, 2, rank, d // 8), F32),
            pltpu.VMEM((m, d), BF16),
            pltpu.VMEM((m, fh), BF16),
            pltpu.VMEM((RING, d, TILE), BF16),
            pltpu.VMEM((d, rank), BF16),
            pltpu.VMEM((rank, fh), BF16),
            pltpu.VMEM((fh, rank), BF16),
            pltpu.VMEM((rank, d), BF16),
            pltpu.VMEM((2, m, w), F32),
            pltpu.VMEM((4, m // 2, w), F32),
            pltpu.VMEM((nb, m // 2, w), F32),
            pltpu.VMEM((nb, m // 4, w), F32),
            pltpu.VMEM((nb, m // 8, w), F32),
            pltpu.VMEM((nb, m // 4, w), BF16),
            pltpu.VMEM((2, m // 8, d), BF16),
            dma((RING,)), dma((RING,)), dma((2,)), dma((2,)), dma((18,)), dma((10,)), dma((3,)),
            dma((2,)), dma((4,)), dma((nb,)), dma((nb,)), dma((nb,)), dma((nb,)), dma((nb,)), dma((nb,)),
            dma((nb,)), dma((nb,)), dma((4,)),
            pltpu.SemaphoreType.REGULAR, pltpu.SemaphoreType.REGULAR,
            pltpu.SemaphoreType.REGULAR, pltpu.SemaphoreType.REGULAR,
        ],
        compiler_params=pltpu.CompilerParams(has_side_effects=True, vmem_limit_bytes=67043328),
        name='mlp_ring',
    )(base_up, base_down, *factors, learn_rate, prompts)
    return hid, tail, near


def solution(mesh):
    left_spec = P('pool', None, 'tp', None)
    right_spec = P('pool', None, None, 'tp')
    prompt_spec = P('pool', None, None)

    def local_step(base_up, base_down, up_left, up_right, down_left, down_right, grad_up_left, grad_up_right, grad_down_left, grad_down_right, learn_rate, prompts):
        step_size = learn_rate[0]
        t, core = lax.axis_index('tp'), lax.axis_index('pool')
        xb, yb = t % 2, t // 2
        factors = (up_left, grad_up_left, up_right, grad_up_right, down_left, grad_down_left, down_right, grad_down_right)
        hid, tail, near = fused_mlp(base_up, base_down, factors, learn_rate, prompts)
        from_x = lax.ppermute(tail, ('tp', 'pool'), [(2 * n, 2 * (n ^ 1) + 1) for n in range(4)])
        from_y = lax.ppermute(tail, ('tp', 'pool'), [(2 * n + 1, 2 * (n ^ 2) + 1) for n in range(4)])
        trainer = core == 0
        head = jnp.where(trainer, jnp.zeros_like(hid), hid)[None]
        new = [jnp.where(trainer, value - step_size * grad, jnp.zeros_like(value))
               for value, grad in zip(factors[::2], factors[1::2])]
        new_up_left, new_up_right, new_down_left, new_down_right = new
        last = jnp.concatenate([jnp.where(xb == 0, near, from_x), jnp.where(xb == 0, from_x, near),
                                jnp.where(yb == 0, tail, from_y), jnp.where(yb == 0, from_y, tail)], axis=0)
        last = jnp.where(trainer, jnp.zeros_like(last), last)[None]
        head = lax.optimization_barrier(head)
        hidden_out = lax.dynamic_update_slice(head, last, (0, hid.shape[0] - last.shape[1], 0))
        return new_up_left, new_up_right, new_down_left, new_down_right, hidden_out

    return jax.shard_map(local_step, mesh=mesh,
                         in_specs=(P(None, None, 'tp'), P(None, 'tp', None), left_spec, right_spec, left_spec, right_spec, left_spec, right_spec, left_spec, right_spec, P(None), prompt_spec),
                         out_specs=(left_spec, right_spec, left_spec, right_spec, prompt_spec),
                         check_vma=False)
```

```python
import functools

import jax
import jax.numpy as jnp
from jax import lax
from jax.experimental import pallas as pl
from jax.experimental.pallas import tpu as pltpu
from jax.sharding import PartitionSpec as P

CHUNK = 512
TILE = 256
RING = 3
LAG = (2, 4, 7, 23)
BF16 = jnp.bfloat16
F32 = jnp.float32
MESH = pl.DeviceIdType.MESH


def mlp_kernel(dims, base_up, base_dn, a_up, a_up_g, b_up, b_up_g, a_dn, a_dn_g, b_dn, b_dn_g, rate, prompts, hid, tail, near, wm,
               left, right, x, u, wb, aup, bup, adn, bdn, pb, rx0, s1, rx1, rx2, ob, res,
               wsem, osem, lsem, rsem, asend, arecv, xsem, s0, r0, ss1, rs1, ss2, rs2, ss3, rs3, ss4, ss5, fsem,
               xfree, cr1, cr2, cr3):
    m, nc, nb, d, fh, w = dims
    total = nc * nb
    ring = nb
    halves = w // TILE
    mh, mq, me = m // 2, m // 4, m // 8
    d4 = d // 4
    rank = aup.shape[1]
    t = lax.axis_index('tp')
    c = lax.axis_index('pool')
    xb, yb = t % 2, t // 2
    near_x, near_y = t + 1 - 2 * xb, t + 2 - 4 * yb
    b1 = (1 - c) * xb + c * yb
    b2 = c * xb + (1 - c) * yb
    p1 = (1 - c) * near_x + c * near_y
    p2 = c * near_x + (1 - c) * near_y

    def rows(start, size):
        return pl.ds(pl.multiple_of(start, size), size)

    def remote(src, dst, send, recv, device):
        return pltpu.make_async_remote_copy(src_ref=src, dst_ref=dst, send_sem=send, recv_sem=recv,
                                            device_id=device, device_id_type=MESH)

    def base_loads(r, slot):
        @pl.when(r < nb)
        def _():
            pltpu.make_async_copy(base_up.at[0, :, rows(c * fh + r * TILE, TILE)], wb.at[slot], wsem.at[slot]).start()

        @pl.when(r >= nb)
        def _():
            for h in range(halves):
                pltpu.make_async_copy(base_dn.at[0, rows(c * fh, fh), rows((r - nb) * w + h * TILE, TILE)],
                                      wb.at[slot, pl.ds(h * fh, fh), :], wsem.at[slot]).start()

    def merged_load(r, slot):
        return pltpu.make_async_copy(wm.at[r], wb.at[slot], wsem.at[slot])

    def merged_store(r, slot):
        return pltpu.make_async_copy(wb.at[slot], wm.at[r], osem.at[slot])

    piece = min(512, fh)

    def merge_up(slot, j):
        right = bup[:, rows(j * TILE, TILE)]
        for q in range(d // piece):
            part = pl.ds(q * piece, piece)
            delta = jnp.dot(aup[part, :], right, preferred_element_type=F32).astype(BF16)
            wb[slot, part, :] = wb[slot, part, :] + delta

    def merge_dn(slot, i):
        for h in range(halves):
            right = bdn[:, rows(i * w + h * TILE, TILE)]
            for q in range(fh // piece):
                delta = jnp.dot(adn[pl.ds(q * piece, piece), :], right, preferred_element_type=F32).astype(BF16)
                part = pl.ds(h * fh + q * piece, piece)
                wb[slot, part, :] = wb[slot, part, :] + delta

    def dot_up(slot, j):
        pre = jnp.dot(x[...], wb[slot], preferred_element_type=F32)
        u[:, rows(j * TILE, TILE)] = jax.nn.gelu(pre, approximate=True).astype(BF16)

    def dot_dn(slot, buf):
        for h in range(halves):
            pb[buf, :, pl.ds(h * TILE, TILE)] = jnp.dot(u[...], wb[slot, pl.ds(h * fh, fh), :],
                                                        preferred_element_type=F32)

    def swap(g):
        return remote(pb.at[g % 2, rows((1 - c) * mh, mh), :], rx0.at[g % 4], s0.at[g % 2], r0.at[g % 4], (t, 1 - c))

    def first(g):
        return remote(s1.at[g % ring, rows((1 - b1) * mq, mq), :], rx1.at[g % ring],
                      ss1.at[g % ring], rs1.at[g % ring], (p1, c))

    def second(g):
        return remote(s1.at[g % ring, rows(b1 * mq + (1 - b2) * me, me), :], rx2.at[g % ring],
                      ss2.at[g % ring], rs2.at[g % ring], (p2, c))

    def gather(g):
        half = ob.at[g % ring, rows(b2 * me, me), :]
        return remote(half, half, ss3.at[g % ring], rs3.at[g % ring], (p2, c))

    def final_place(g):
        return hid.at[rows((g // nb) * m + c * mh + b1 * mq, mq), rows((g % nb) * w, w)]

    def final_far(g):
        return remote(ob.at[g % ring], final_place(g), ss4.at[g % ring], fsem.at[1 + c], (p1, 1))

    def final_near(g):
        return remote(ob.at[g % ring], final_place(g), ss5.at[g % ring], fsem.at[0], (t, 1))

    def final_local(g):
        return pltpu.make_async_copy(ob.at[g % ring], final_place(g), ss5.at[g % ring])

    def stage_a(g):
        slot = g % ring
        swap(g).wait_send()
        swap(g).wait_recv()
        s1[slot] = pb[g % 2, rows(c * mh, mh), :] + rx0[g % 4]

        @pl.when(g >= ring)
        def _():
            pl.semaphore_wait(cr1, 1)
        first(g).start()

    def stage_b(g):
        slot = g % ring
        keep = rows(b1 * mq, mq)
        first(g).wait_recv()
        s1[slot, keep, :] = s1[slot, keep, :] + rx1[slot]

        @pl.when(g + ring < total)
        def _():
            pl.semaphore_signal(cr1, inc=1, device_id=(p1, c), device_id_type=MESH)

        @pl.when(g >= ring)
        def _():
            pl.semaphore_wait(cr2, 1)
        second(g).start()

    def stage_c(g):
        slot = g % ring
        keep = rows(b1 * mq + b2 * me, me)
        second(g).wait_recv()
        first(g).wait_send()
        held = res[(g // nb) % 2, :, rows((g % nb) * w, w)].astype(F32)
        ob[slot, rows(b2 * me, me), :] = (held + (s1[slot, keep, :] + rx2[slot])).astype(BF16)

        @pl.when(g + ring < total)
        def _():
            pl.semaphore_signal(cr2, inc=1, device_id=(p2, c), device_id_type=MESH)

        @pl.when(g >= ring)
        def _():
            pl.semaphore_wait(cr3, 1)
        gather(g).start()

    def tail_local(g):
        return pltpu.make_async_copy(ob.at[g % ring], tail.at[:, rows((g % nb) * w, w)], ss4.at[g % ring])

    def tail_near(g):
        return remote(ob.at[g % ring], near.at[:, rows((g % nb) * w, w)], ss5.at[g % ring], fsem.at[3], (t, 1))

    def stage_d(g):
        gather(g).wait_recv()
        second(g).wait_send()

        @pl.when(g < total - nb)
        def _():
            final_far(g).start()

            @pl.when(c == 0)
            def _():
                final_near(g).start()

            @pl.when(c == 1)
            def _():
                final_local(g).start()

        @pl.when(g >= total - nb)
        def _():
            tail_local(g).start()

            @pl.when(c == 0)
            def _():
                tail_near(g).start()

    def stage_e(g):
        gather(g).wait_send()

        @pl.when(g < total - nb)
        def _():
            final_far(g).wait_send()

            @pl.when(c == 0)
            def _():
                final_near(g).wait_send()

            @pl.when(c == 1)
            def _():
                final_local(g).wait()

        @pl.when(g >= total - nb)
        def _():
            tail_local(g).wait()

            @pl.when(c == 0)
            def _():
                tail_near(g).wait_send()

        @pl.when(g + ring < total)
        def _():
            pl.semaphore_signal(cr3, inc=1, device_id=(p2, c), device_id_type=MESH)

    def stages(s):
        before = s - 1
        r = before % (2 * nb)

        @pl.when((r >= nb) & (before < 2 * nb * nc))
        def _():
            stage_a((before // (2 * nb)) * nb + r - nb)
        for lag, stage in zip(LAG, (stage_b, stage_c, stage_d, stage_e)):
            late = s - nb - lag

            @pl.when((late >= 0) & (late % 2 == 0) & (late < 2 * total))
            def _():
                stage(late // 2)

    def x_load(k):
        return pltpu.make_async_copy(prompts.at[0, rows(k * m, m), :], x, xsem.at[0])

    def x_send():
        return remote(x, x, xsem.at[1], xsem.at[2], (t, 0))

    def keep_rows(k):
        res[k % 2] = x[rows(c * mh + b1 * mq + b2 * me, me), :]

    def up_piece(owner):
        return aup.at[rows(owner * d4, d4), :]

    def dn_piece(owner):
        return bdn.at[:, rows(owner * d4, d4)]

    others = (near_x, near_y, 3 - t)

    def up_out(n):
        return remote(up_piece(t), up_piece(t), asend.at[n], arecv.at[t], (others[n], 0))

    def dn_out(n):
        return remote(dn_piece(t), dn_piece(t), asend.at[3 + n], arecv.at[4 + t], (others[n], 0))

    def up_in(owner):
        return remote(up_piece(owner), up_piece(owner), asend.at[6], arecv.at[owner], (t, 1))

    def dn_in(owner):
        return remote(dn_piece(owner), dn_piece(owner), asend.at[7], arecv.at[4 + owner], (t, 1))

    def pass_up(n):
        return remote(up_piece(others[n]), up_piece(others[n]), asend.at[8 + n], arecv.at[others[n]], (t, 1))

    def pass_dn(n):
        return remote(dn_piece(others[n]), dn_piece(others[n]), asend.at[11 + n], arecv.at[4 + others[n]], (t, 1))

    far_b = u.at[pl.ds(0, rank), :]
    far_a = wb.at[2, pl.ds(0, fh), pl.ds(0, rank)]
    own = (
        lambda: remote(up_piece(t), up_piece(t), asend.at[14], arecv.at[t], (t, 1)),
        lambda: remote(far_b, bup, asend.at[15], arecv.at[8], (t, 1)),
        lambda: remote(far_a, adn, asend.at[16], arecv.at[9], (t, 1)),
        lambda: remote(dn_piece(t), dn_piece(t), asend.at[17], arecv.at[4 + t], (t, 1)),
    )

    size = d4 // 2
    lefts = [(a_up, a_up_g, q, aup, t * d4 + q * size) for q in range(2)]
    lefts += [(a_dn, a_dn_g, q, adn, q * size) for q in range(4)]
    lefts += [(a_dn, a_dn_g, 4 + q, None, q * size) for q in range(4)]
    rights = [(b_up, b_up_g, q, bup, q * size) for q in range(4)]
    rights += [(b_up, b_up_g, 4 + q, u, q * size) for q in range(4)]
    rights += [(b_dn, b_dn_g, q, bdn, t * d4 + q * size) for q in range(2)]

    def left_load(n):
        value, grad, q, _, _ = lefts[n]
        for side, src in enumerate((value, grad)):
            pltpu.make_async_copy(src.at[0, 0, pl.ds(q * size, size), :], left.at[n % 2, side], lsem.at[n % 2]).start()

    def right_load(n):
        value, grad, q, _, _ = rights[n]
        for side, src in enumerate((value, grad)):
            pltpu.make_async_copy(src.at[0, 0, :, pl.ds(q * size, size)], right.at[n % 2, side], rsem.at[n % 2]).start()

    def left_update(n):
        _, _, _, dst, start = lefts[n]
        pltpu.make_async_copy(left.at[n % 2], left.at[n % 2], lsem.at[n % 2]).wait()
        new = (left[n % 2, 0] - rate[0] * left[n % 2, 1]).astype(BF16)
        if dst is None:
            wb[2, rows(start, size), pl.ds(0, rank)] = new
        else:
            dst[rows(start, size), :] = new
        if n + 2 < len(lefts):
            left_load(n + 2)

    def right_update(n):
        _, _, _, dst, start = rights[n]
        pltpu.make_async_copy(right.at[n % 2], right.at[n % 2], rsem.at[n % 2]).wait()
        new = (right[n % 2, 0] - rate[0] * right[n % 2, 1]).astype(BF16)
        if dst is u:
            u[pl.ds(0, rank), rows(start, size)] = new
        else:
            dst[:, rows(start, size)] = new
        if n + 2 < len(rights):
            right_load(n + 2)

    @pl.when(c == 0)
    def _():
        for n in range(2):
            left_load(n)
        for n in range(2):
            right_load(n)
        base_loads(0, 0)
        base_loads(1, 1)
        for n in range(2):
            left_update(n)
        for n in range(3):
            up_out(n).start()
        own[0]().start()
        for n in range(8):
            right_update(n)
        own[1]().start()
        for n in range(8, 10):
            right_update(n)
        for n in range(3):
            dn_out(n).start()
        own[3]().start()
        for n in range(2, 10):
            left_update(n)
        own[2]().start()
        for n in range(3):
            up_in(others[n]).wait_recv()
            pass_up(n).start()
        own[1]().wait_send()
        own[2]().wait_send()
        x_send().wait_recv()

    @pl.when(c == 1)
    def _():
        x_load(0).start()
        base_loads(0, 0)
        base_loads(1, 1)
        x_load(0).wait()
        x_send().start()
        for owner in range(4):
            up_in(owner).wait_recv()
        own[1]().wait_recv()

    merged_load(0, 0).wait()
    merge_up(0, 0)
    keep_rows(0)

    def tile_turn(r):
        merged_store(r, r % RING).start()

        @pl.when(r >= 1)
        def _():
            merged_store(r - 1, (r + 2) % RING).wait()

        @pl.when(r + 2 < 2 * nb)
        def _():
            base_loads(r + 2, (r + 2) % RING)

        @pl.when(r + 2 >= 2 * nb)
        def _():
            merged_load(r + 2 - 2 * nb, (r + 2) % RING).start()

        merged_load(0, (r + 1) % RING).wait()

    def first_up(r, carry):
        @pl.when(r == nb // 2)
        def _():
            @pl.when(c == 0)
            def _():
                for n in range(3):
                    dn_in(others[n]).wait_recv()
                    pass_dn(n).start()
        tile_turn(r)
        dot_up(r % RING, r)

        @pl.when(r < nb)
        def _():
            merge_up((r + 1) % RING, r + 1)
        return carry

    lax.fori_loop(0, nb - 1, first_up, 0)

    @pl.when(c == 0)
    def _():
        for n in range(3):
            up_out(n).wait_send()
            dn_out(n).wait_send()
            pass_up(n).wait_send()
            pass_dn(n).wait_send()
        own[0]().wait_send()
        own[3]().wait_send()

    @pl.when(c == 1)
    def _():
        for owner in range(4):
            dn_in(owner).wait_recv()
        own[2]().wait_recv()

    tile_turn(nb - 1)
    merge_dn(nb % RING, 0)
    dot_up((nb - 1) % RING, nb - 1)

    def x_turn(k, r):
        @pl.when((k + 1 < nc) & (c == 0) & (r == nb))
        def _():
            pl.semaphore_signal(xfree, inc=1, device_id=(t, 1), device_id_type=MESH)

        @pl.when((k + 1 < nc) & (c == 1) & (r == nb))
        def _():
            @pl.when(k >= 0)
            def _():
                x_send().wait_send()
            x_load(k + 1).start()

        @pl.when((k + 1 < nc) & (c == 1) & (r == nb + 2))
        def _():
            x_load(k + 1).wait()
            pl.semaphore_wait(xfree, 1)
            x_send().start()

        @pl.when((k >= 1) & (r == 0))
        def _():
            @pl.when(c == 0)
            def _():
                x_send().wait_recv()
            keep_rows(k)

    def first_dn(r, carry):
        x_turn(0, r)
        tile_turn(r)
        dot_dn(r % RING, r % 2)
        merge_dn((r + 1) % RING, r + 1 - nb)
        swap(r - nb).start()
        stages(r)
        return carry

    lax.fori_loop(nb, 2 * nb - 1, first_dn, 0)

    def step(s, carry):
        k, r = s // (2 * nb), s % (2 * nb)
        x_turn(k, r)

        @pl.when(s == 2 * nb - 1)
        def _():
            tile_turn(2 * nb - 1)

        @pl.when(s == 2 * nb)
        def _():
            merged_store(2 * nb - 1, (2 * nb - 1) % RING).wait()

        @pl.when(s >= 2 * nb)
        def _():
            @pl.when(s + 2 < 2 * nb * nc)
            def _():
                merged_load((s + 2) % (2 * nb), (s + 2) % RING).start()

            @pl.when(s > 2 * nb)
            def _():
                merged_load(0, s % RING).wait()

        @pl.when(r < nb)
        def _():
            dot_up(s % RING, r)

        @pl.when(r >= nb)
        def _():
            dot_dn(s % RING, s % 2)
            swap(k * nb + r - nb).start()
        stages(s)
        return carry

    lax.fori_loop(2 * nb - 1, 2 * nb * nc, step, 0)

    def drain(s, carry):
        stages(s)
        return carry

    lax.fori_loop(2 * nb * nc, 2 * (total - 1) + nb + LAG[-1] + 1, drain, 0)

    @pl.when(c == 1)
    def _():
        x_send().wait_send()
        for n in range(3):
            part = hid.at[pl.ds(0, (nc - 1) * mq), :]
            pltpu.make_async_copy(part, part, fsem.at[n]).wait()
        pltpu.make_async_copy(near, near, fsem.at[3]).wait()


def fused_mlp(base_up, base_down, factors, learn_rate, prompts):
    tokens, d = prompts.shape[1:]
    fh = base_up.shape[2] // 2
    nb = fh // TILE
    w = d // nb
    m = min(CHUNK, tokens)
    nc = tokens // m
    rank = factors[0].shape[3]
    dims = (m, nc, nb, d, fh, w)
    dma = pltpu.SemaphoreType.DMA
    anywhere = pl.BlockSpec(memory_space=pl.ANY)
    hid, tail, near, _ = pl.pallas_call(
        functools.partial(mlp_kernel, dims),
        out_shape=(jax.ShapeDtypeStruct((tokens, d), BF16), jax.ShapeDtypeStruct((m // 4, d), BF16),
                   jax.ShapeDtypeStruct((m // 4, d), BF16), jax.ShapeDtypeStruct((2 * nb, d, TILE), BF16)),
        in_specs=[anywhere] * 10 + [pl.BlockSpec(memory_space=pltpu.SMEM), anywhere],
        out_specs=(anywhere,) * 4,
        scratch_shapes=[
            pltpu.VMEM((2, 2, d // 8, rank), F32),
            pltpu.VMEM((2, 2, rank, d // 8), F32),
            pltpu.VMEM((m, d), BF16),
            pltpu.VMEM((m, fh), BF16),
            pltpu.VMEM((RING, d, TILE), BF16),
            pltpu.VMEM((d, rank), BF16),
            pltpu.VMEM((rank, fh), BF16),
            pltpu.VMEM((fh, rank), BF16),
            pltpu.VMEM((rank, d), BF16),
            pltpu.VMEM((2, m, w), F32),
            pltpu.VMEM((4, m // 2, w), F32),
            pltpu.VMEM((nb, m // 2, w), F32),
            pltpu.VMEM((nb, m // 4, w), F32),
            pltpu.VMEM((nb, m // 8, w), F32),
            pltpu.VMEM((nb, m // 4, w), BF16),
            pltpu.VMEM((2, m // 8, d), BF16),
            dma((RING,)), dma((RING,)), dma((2,)), dma((2,)), dma((18,)), dma((10,)), dma((3,)),
            dma((2,)), dma((4,)), dma((nb,)), dma((nb,)), dma((nb,)), dma((nb,)), dma((nb,)), dma((nb,)),
            dma((nb,)), dma((nb,)), dma((4,)),
            pltpu.SemaphoreType.REGULAR, pltpu.SemaphoreType.REGULAR,
            pltpu.SemaphoreType.REGULAR, pltpu.SemaphoreType.REGULAR,
        ],
        compiler_params=pltpu.CompilerParams(has_side_effects=True, vmem_limit_bytes=67043328),
        name='mlp_ring',
    )(base_up, base_down, *factors, learn_rate, prompts)
    return hid, tail, near


def finish_kernel(dims, hid, tail, near, a_up, a_up_g, b_up, b_up_g, a_dn, a_dn_g, b_dn, b_dn_g, rate,
                  out, a_up_n, b_up_n, a_dn_n, b_dn_n, buf, left, right, left_n, right_n, isem, osem, lsem, rsem, lnsem, rnsem):
    tokens, d, m, step = dims
    t = lax.axis_index('tp')
    c = lax.axis_index('pool')
    xb, yb = t % 2, t // 2
    mq = m // 4
    head = tokens - m
    slots = buf.shape[0]
    ahead = slots // 2
    size = d // 8

    lefts = [(a_up, a_up_g, a_up_n, q) for q in range(2)] + [(a_dn, a_dn_g, a_dn_n, q) for q in range(8)]
    rights = [(b_dn, b_dn_g, b_dn_n, q) for q in range(2)] + [(b_up, b_up_g, b_up_n, q) for q in range(8)]

    def left_piece(ref, q):
        return ref.at[0, 0, pl.ds(q * size, size), :]

    def right_piece(ref, q):
        return ref.at[0, 0, :, pl.ds(q * size, size)]

    def left_store(n, slot):
        return pltpu.make_async_copy(left_n.at[slot], left_piece(lefts[n][2], lefts[n][3]), lnsem.at[slot])

    def right_store(n, slot):
        return pltpu.make_async_copy(right_n.at[slot], right_piece(rights[n][2], rights[n][3]), rnsem.at[slot])

    @pl.when(c == 1)
    def _():
        moves = [(hid, q * step, q * step) for q in range(head // step)]
        moves += [(near, q * step, head + xb * mq + q * step) for q in range(mq // step)]
        moves += [(tail, q * step, head + 2 * mq + yb * mq + q * step) for q in range(mq // step)]

        def load(n):
            src, start, _ = moves[n]
            return pltpu.make_async_copy(src.at[pl.ds(start, step), :], buf.at[n % slots], isem.at[n % slots])

        def store(n):
            start = moves[n][2]
            return pltpu.make_async_copy(buf.at[n % slots], out.at[0, pl.ds(pl.multiple_of(start, step), step), :], osem.at[n % slots])

        for n in range(ahead):
            load(n).start()
        left_n[0] = jnp.zeros_like(left_n[0])
        right_n[0] = jnp.zeros_like(right_n[0])
        for n in range(len(moves)):
            load(n).wait()
            store(n).start()
            if n < 10:
                left_store(n, 0).start()
                right_store(n, 0).start()
            if n >= ahead:
                store(n - ahead).wait()
            if n + ahead < len(moves):
                load(n + ahead).start()
        for n in range(len(moves) - ahead, len(moves)):
            store(n).wait()
        for n in range(10):
            left_store(n, 0).wait()
            right_store(n, 0).wait()

    @pl.when(c == 0)
    def _():
        def left_load(n):
            for side in range(2):
                pltpu.make_async_copy(left_piece(lefts[n][side], lefts[n][3]), left.at[n % 2, side], lsem.at[n % 2]).start()

        def right_load(n):
            for side in range(2):
                pltpu.make_async_copy(right_piece(rights[n][side], rights[n][3]), right.at[n % 2, side], rsem.at[n % 2]).start()

        def blank(n):
            return pltpu.make_async_copy(buf.at[0], out.at[0, pl.ds(n * step, step), :], osem.at[0])

        for n in range(2):
            left_load(n)
            right_load(n)
        buf[0] = jnp.zeros_like(buf[0])
        blanks = tokens // step
        for n in range(10):
            pltpu.make_async_copy(left.at[n % 2], left.at[n % 2], lsem.at[n % 2]).wait()
            pltpu.make_async_copy(right.at[n % 2], right.at[n % 2], rsem.at[n % 2]).wait()
            if n >= 2:
                left_store(n - 2, n % 2).wait()
                right_store(n - 2, n % 2).wait()
            left_n[n % 2] = left[n % 2, 0] - rate[0] * left[n % 2, 1]
            right_n[n % 2] = right[n % 2, 0] - rate[0] * right[n % 2, 1]
            left_store(n, n % 2).start()
            right_store(n, n % 2).start()
            if n + 2 < 10:
                left_load(n + 2)
                right_load(n + 2)
            for q in range(n * blanks // 10, (n + 1) * blanks // 10):
                blank(q).start()
        for n in range(8, 10):
            left_store(n, n % 2).wait()
            right_store(n, n % 2).wait()
        for q in range(blanks):
            blank(q).wait()


def finish(hid, tail, near, factors, learn_rate, m):
    tokens, d = hid.shape
    rank = factors[0].shape[3]
    step = min(64, m // 4)
    dma = pltpu.SemaphoreType.DMA
    anywhere = pl.BlockSpec(memory_space=pl.ANY)
    return pl.pallas_call(
        functools.partial(finish_kernel, (tokens, d, m, step)),
        out_shape=(jax.ShapeDtypeStruct((1, tokens, d), BF16),) + tuple(jax.ShapeDtypeStruct(f.shape, F32) for f in factors[::2]),
        in_specs=[anywhere] * 11 + [pl.BlockSpec(memory_space=pltpu.SMEM)],
        out_specs=(anywhere,) * 5,
        scratch_shapes=[
            pltpu.VMEM((8, step, d), BF16),
            pltpu.VMEM((2, 2, d // 8, rank), F32),
            pltpu.VMEM((2, 2, rank, d // 8), F32),
            pltpu.VMEM((2, d // 8, rank), F32),
            pltpu.VMEM((2, rank, d // 8), F32),
            dma((8,)), dma((8,)), dma((2,)), dma((2,)), dma((2,)), dma((2,)),
        ],
        compiler_params=pltpu.CompilerParams(vmem_limit_bytes=67043328),
        cost_estimate=pl.CostEstimate(flops=20_000_000_000, bytes_accessed=70_000_000, transcendentals=0),
        name='finish',
    )(hid, tail, near, *factors, learn_rate)


def solution(mesh):
    left_spec = P('pool', None, 'tp', None)
    right_spec = P('pool', None, None, 'tp')
    prompt_spec = P('pool', None, None)

    def local_step(base_up, base_down, up_left, up_right, down_left, down_right, grad_up_left, grad_up_right, grad_down_left, grad_down_right, learn_rate, prompts):
        t = lax.axis_index('tp')
        xb, yb = t % 2, t // 2
        factors = (up_left, grad_up_left, up_right, grad_up_right, down_left, grad_down_left, down_right, grad_down_right)
        m = min(CHUNK, prompts.shape[1])
        hid, tail, near = fused_mlp(base_up, base_down, factors, learn_rate, prompts)
        from_x = lax.ppermute(tail, ('tp', 'pool'), [(2 * n, 2 * (n ^ 1) + 1) for n in range(4)])
        from_y = lax.ppermute(tail, ('tp', 'pool'), [(2 * n + 1, 2 * (n ^ 2) + 1) for n in range(4)])
        hidden_out, new_up_left, new_up_right, new_down_left, new_down_right = finish(hid, tail, near, factors, learn_rate, m)
        start = hid.shape[0] - m
        hidden_out = lax.dynamic_update_slice(hidden_out, from_x[None], (0, start + (1 - xb) * (m // 4), 0))
        hidden_out = lax.dynamic_update_slice(hidden_out, from_y[None], (0, start + m // 2 + (1 - yb) * (m // 4), 0))
        return new_up_left, new_up_right, new_down_left, new_down_right, hidden_out

    return jax.shard_map(local_step, mesh=mesh,
                         in_specs=(P(None, None, 'tp'), P(None, 'tp', None), left_spec, right_spec, left_spec, right_spec, left_spec, right_spec, left_spec, right_spec, P(None), prompt_spec),
                         out_specs=(left_spec, right_spec, left_spec, right_spec, prompt_spec),
                         check_vma=False)
```

```python
import functools

import jax
import jax.numpy as jnp
from jax import lax
from jax.experimental import pallas as pl
from jax.experimental.pallas import tpu as pltpu
from jax.sharding import PartitionSpec as P

CHUNK = 512
TILE = 256
RING = 3
LAG = (2, 4, 7, 23)
BF16 = jnp.bfloat16
F32 = jnp.float32
MESH = pl.DeviceIdType.MESH


def mlp_kernel(dims, base_up, base_dn, a_up, a_up_g, b_up, b_up_g, a_dn, a_dn_g, b_dn, b_dn_g, rate, prompts, hid, tail, near, wm,
               left, right, far_a, x, u, wb, aup, bup, adn, bdn, pb, rx0, s1, rx1, rx2, ob, res,
               wsem, osem, lsem, rsem, qload, qstore, asend, arecv, xsem, xqsem, s0, r0, ss1, rs1, ss2, rs2, ss3, rs3, ss4, ss5, fsem,
               xfree, cr1, cr2, cr3):
    m, nc, nb, d, fh, w = dims
    total = nc * nb
    ring = nb
    halves = w // TILE
    mh, mq, me = m // 2, m // 4, m // 8
    d4 = d // 4
    rank = aup.shape[1]
    t = lax.axis_index('tp')
    c = lax.axis_index('pool')
    xb, yb = t % 2, t // 2
    near_x, near_y = t + 1 - 2 * xb, t + 2 - 4 * yb
    b1 = (1 - c) * xb + c * yb
    b2 = c * xb + (1 - c) * yb
    p1 = (1 - c) * near_x + c * near_y
    p2 = c * near_x + (1 - c) * near_y
    others = (near_x, near_y, 3 - t)

    def rows(start, size):
        return pl.ds(pl.multiple_of(start, size), size)

    def remote(src, dst, send, recv, device):
        return pltpu.make_async_remote_copy(src_ref=src, dst_ref=dst, send_sem=send, recv_sem=recv,
                                            device_id=device, device_id_type=MESH)

    def base_loads(r, slot):
        @pl.when(r < nb)
        def _():
            for q in others:
                pltpu.make_async_copy(base_up.at[0, rows(q * d4, d4), rows(c * fh + r * TILE, TILE)],
                                      wb.at[slot, rows(q * d4, d4), :], wsem.at[slot]).start()

        @pl.when(r >= nb)
        def _():
            for h in range(halves):
                pltpu.make_async_copy(base_dn.at[0, rows(c * fh, fh), rows((r - nb) * w + h * TILE, TILE)],
                                      wb.at[slot, pl.ds(h * fh, fh), :], wsem.at[slot]).start()

    def up_wait(slot):
        part = wb.at[slot, pl.ds(0, 3 * d4), :]
        pltpu.make_async_copy(part, part, wsem.at[slot]).wait()

    def up_store(r, slot):
        for q in others:
            pltpu.make_async_copy(wb.at[slot, rows(q * d4, d4), :], wm.at[r, rows(q * d4, d4), :], osem.at[slot]).start()

    def up_store_wait(slot):
        part = wb.at[slot, pl.ds(0, 3 * d4), :]
        pltpu.make_async_copy(part, part, osem.at[slot]).wait()

    def merged_load(r, slot):
        return pltpu.make_async_copy(wm.at[r], wb.at[slot], wsem.at[slot])

    def merged_store(r, slot):
        return pltpu.make_async_copy(wb.at[slot], wm.at[r], osem.at[slot])

    piece = min(512, d4)

    def merge_up(slot, j):
        cols = bup[:, rows(j * TILE, TILE)]
        for q in others:
            for n in range(d4 // piece):
                part = rows(q * d4 + n * piece, piece)
                delta = jnp.dot(aup[part, :], cols, preferred_element_type=F32).astype(BF16)
                wb[slot, part, :] = wb[slot, part, :] + delta

    def own_rows(j):
        return wb.at[RING - 1, rows((j % 4) * d4, d4), :]

    def own_load(j):
        return pltpu.make_async_copy(base_up.at[0, rows(t * d4, d4), rows(c * fh + j * TILE, TILE)], own_rows(j), qload.at[j % 4])

    def own_store(j):
        return pltpu.make_async_copy(own_rows(j), wm.at[j, rows(t * d4, d4), :], qstore.at[j % 4])

    def own_merge(j):
        cols = bup[:, rows(j * TILE, TILE)]
        for n in range(d4 // piece):
            part = rows((j % 4) * d4 + n * piece, piece)
            delta = jnp.dot(aup[rows(t * d4 + n * piece, piece), :], cols, preferred_element_type=F32).astype(BF16)
            wb[RING - 1, part, :] = wb[RING - 1, part, :] + delta

    def own_dot(j):
        pre = jnp.dot(x[:, rows(t * d4, d4)], wb[RING - 1, rows((j % 4) * d4, d4), :], preferred_element_type=F32)
        s1[j, :, pl.ds(0, TILE)] = pre[:mh]
        s1[j, :, pl.ds(TILE, TILE)] = pre[mh:]

    def other_parts(slot, j):
        pre = sum(jnp.dot(x[:, rows(q * d4, d4)], wb[slot, rows(q * d4, d4), :], preferred_element_type=F32) for q in others)
        top = pre[:mh] + s1[j, :, pl.ds(0, TILE)]
        low = pre[mh:] + s1[j, :, pl.ds(TILE, TILE)]
        u[pl.ds(0, mh), rows(j * TILE, TILE)] = jax.nn.gelu(top, approximate=True).astype(BF16)
        u[pl.ds(mh, mh), rows(j * TILE, TILE)] = jax.nn.gelu(low, approximate=True).astype(BF16)

    def merge_dn(slot, i):
        for h in range(halves):
            cols = bdn[:, rows(i * w + h * TILE, TILE)]
            for q in range(fh // piece):
                delta = jnp.dot(adn[pl.ds(q * piece, piece), :], cols, preferred_element_type=F32).astype(BF16)
                part = pl.ds(h * fh + q * piece, piece)
                wb[slot, part, :] = wb[slot, part, :] + delta

    def dot_up(slot, j):
        pre = jnp.dot(x[...], wb[slot], preferred_element_type=F32)
        u[:, rows(j * TILE, TILE)] = jax.nn.gelu(pre, approximate=True).astype(BF16)

    def dot_dn(slot, buf):
        for h in range(halves):
            pb[buf, :, pl.ds(h * TILE, TILE)] = jnp.dot(u[...], wb[slot, pl.ds(h * fh, fh), :],
                                                        preferred_element_type=F32)

    def swap(g):
        return remote(pb.at[g % 2, rows((1 - c) * mh, mh), :], rx0.at[g % 4], s0.at[g % 2], r0.at[g % 4], (t, 1 - c))

    def first(g):
        return remote(s1.at[g % ring, rows((1 - b1) * mq, mq), :], rx1.at[g % ring],
                      ss1.at[g % ring], rs1.at[g % ring], (p1, c))

    def second(g):
        return remote(s1.at[g % ring, rows(b1 * mq + (1 - b2) * me, me), :], rx2.at[g % ring],
                      ss2.at[g % ring], rs2.at[g % ring], (p2, c))

    def gather(g):
        half = ob.at[g % ring, rows(b2 * me, me), :]
        return remote(half, half, ss3.at[g % ring], rs3.at[g % ring], (p2, c))

    def final_place(g):
        return hid.at[rows((g // nb) * m + c * mh + b1 * mq, mq), rows((g % nb) * w, w)]

    def final_far(g):
        return remote(ob.at[g % ring], final_place(g), ss4.at[g % ring], fsem.at[1 + c], (p1, 1))

    def final_near(g):
        return remote(ob.at[g % ring], final_place(g), ss5.at[g % ring], fsem.at[0], (t, 1))

    def final_local(g):
        return pltpu.make_async_copy(ob.at[g % ring], final_place(g), ss5.at[g % ring])

    def stage_a(g):
        slot = g % ring
        swap(g).wait_send()
        swap(g).wait_recv()
        s1[slot] = pb[g % 2, rows(c * mh, mh), :] + rx0[g % 4]

        @pl.when(g >= ring)
        def _():
            pl.semaphore_wait(cr1, 1)
        first(g).start()

    def stage_b(g):
        slot = g % ring
        keep = rows(b1 * mq, mq)
        first(g).wait_recv()
        s1[slot, keep, :] = s1[slot, keep, :] + rx1[slot]

        @pl.when(g + ring < total)
        def _():
            pl.semaphore_signal(cr1, inc=1, device_id=(p1, c), device_id_type=MESH)

        @pl.when(g >= ring)
        def _():
            pl.semaphore_wait(cr2, 1)
        second(g).start()

    def stage_c(g):
        slot = g % ring
        keep = rows(b1 * mq + b2 * me, me)
        second(g).wait_recv()
        first(g).wait_send()
        held = res[(g // nb) % 2, :, rows((g % nb) * w, w)].astype(F32)
        ob[slot, rows(b2 * me, me), :] = (held + (s1[slot, keep, :] + rx2[slot])).astype(BF16)

        @pl.when(g + ring < total)
        def _():
            pl.semaphore_signal(cr2, inc=1, device_id=(p2, c), device_id_type=MESH)

        @pl.when(g >= ring)
        def _():
            pl.semaphore_wait(cr3, 1)
        gather(g).start()

    def tail_local(g):
        return pltpu.make_async_copy(ob.at[g % ring], tail.at[:, rows((g % nb) * w, w)], ss4.at[g % ring])

    def tail_near(g):
        return remote(ob.at[g % ring], near.at[:, rows((g % nb) * w, w)], ss5.at[g % ring], fsem.at[3], (t, 1))

    def stage_d(g):
        gather(g).wait_recv()
        second(g).wait_send()

        @pl.when(g < total - nb)
        def _():
            final_far(g).start()

            @pl.when(c == 0)
            def _():
                final_near(g).start()

            @pl.when(c == 1)
            def _():
                final_local(g).start()

        @pl.when(g >= total - nb)
        def _():
            tail_local(g).start()

            @pl.when(c == 0)
            def _():
                tail_near(g).start()

    def stage_e(g):
        gather(g).wait_send()

        @pl.when(g < total - nb)
        def _():
            final_far(g).wait_send()

            @pl.when(c == 0)
            def _():
                final_near(g).wait_send()

            @pl.when(c == 1)
            def _():
                final_local(g).wait()

        @pl.when(g >= total - nb)
        def _():
            tail_local(g).wait()

            @pl.when(c == 0)
            def _():
                tail_near(g).wait_send()

        @pl.when(g + ring < total)
        def _():
            pl.semaphore_signal(cr3, inc=1, device_id=(p2, c), device_id_type=MESH)

    def stages(s):
        before = s - 1
        r = before % (2 * nb)

        @pl.when((r >= nb) & (before < 2 * nb * nc))
        def _():
            stage_a((before // (2 * nb)) * nb + r - nb)
        for lag, stage in zip(LAG, (stage_b, stage_c, stage_d, stage_e)):
            late = s - nb - lag

            @pl.when((late >= 0) & (late % 2 == 0) & (late < 2 * total))
            def _():
                stage(late // 2)

    def x_load(k):
        return pltpu.make_async_copy(prompts.at[0, rows(k * m, m), :], x, xsem.at[0])

    def x_send():
        return remote(x, x, xsem.at[1], xsem.at[2], (t, 0))

    def keep_rows(k):
        res[k % 2] = x[rows(c * mh + b1 * mq + b2 * me, me), :]

    def up_piece(owner):
        return aup.at[rows(owner * d4, d4), :]

    def dn_piece(owner):
        return bdn.at[:, rows(owner * d4, d4)]

    def up_out(n):
        return remote(up_piece(t), up_piece(t), asend.at[n], arecv.at[t], (others[n], 0))

    def dn_out(n):
        return remote(dn_piece(t), dn_piece(t), asend.at[3 + n], arecv.at[4 + t], (others[n], 0))

    def up_in(owner):
        return remote(up_piece(owner), up_piece(owner), asend.at[6], arecv.at[owner], (t, 1))

    def dn_in(owner):
        return remote(dn_piece(owner), dn_piece(owner), asend.at[7], arecv.at[4 + owner], (t, 1))

    def pass_up(n):
        return remote(up_piece(others[n]), up_piece(others[n]), asend.at[8 + n], arecv.at[others[n]], (t, 1))

    def pass_dn(n):
        return remote(dn_piece(others[n]), dn_piece(others[n]), asend.at[11 + n], arecv.at[4 + others[n]], (t, 1))

    far_b = u.at[pl.ds(0, rank), :]
    own = (
        lambda: remote(up_piece(t), up_piece(t), asend.at[14], arecv.at[t], (t, 1)),
        lambda: remote(far_b, bup, asend.at[15], arecv.at[8], (t, 1)),
        lambda: remote(far_a, adn, asend.at[16], arecv.at[9], (t, 1)),
        lambda: remote(dn_piece(t), dn_piece(t), asend.at[17], arecv.at[4 + t], (t, 1)),
    )

    size = d4 // 2
    lefts = [(a_up, a_up_g, q, aup, t * d4 + q * size) for q in range(2)]
    lefts += [(a_dn, a_dn_g, q, adn, q * size) for q in range(4)]
    lefts += [(a_dn, a_dn_g, 4 + q, far_a, q * size) for q in range(4)]
    rights = [(b_up, b_up_g, q, bup, q * size) for q in range(4)]
    rights += [(b_up, b_up_g, 4 + q, u, q * size) for q in range(4)]
    rights += [(b_dn, b_dn_g, q, bdn, t * d4 + q * size) for q in range(2)]

    def left_load(n):
        value, grad, q, _, _ = lefts[n]
        for side, src in enumerate((value, grad)):
            pltpu.make_async_copy(src.at[0, 0, pl.ds(q * size, size), :], left.at[n % 2, side], lsem.at[n % 2]).start()

    def right_load(n):
        value, grad, q, _, _ = rights[n]
        for side, src in enumerate((value, grad)):
            pltpu.make_async_copy(src.at[0, 0, :, pl.ds(q * size, size)], right.at[n % 2, side], rsem.at[n % 2]).start()

    def left_update(n):
        _, _, _, dst, start = lefts[n]
        pltpu.make_async_copy(left.at[n % 2], left.at[n % 2], lsem.at[n % 2]).wait()
        new = (left[n % 2, 0] - rate[0] * left[n % 2, 1]).astype(BF16)
        dst[rows(start, size), :] = new
        if n + 2 < len(lefts):
            left_load(n + 2)

    def right_update(n):
        _, _, _, dst, start = rights[n]
        pltpu.make_async_copy(right.at[n % 2], right.at[n % 2], rsem.at[n % 2]).wait()
        new = (right[n % 2, 0] - rate[0] * right[n % 2, 1]).astype(BF16)
        if dst is u:
            u[pl.ds(0, rank), rows(start, size)] = new
        else:
            dst[:, rows(start, size)] = new
        if n + 2 < len(rights):
            right_load(n + 2)

    def x_quarter(owner):
        return pltpu.make_async_copy(prompts.at[0, pl.ds(0, m), rows(owner * d4, d4)], x.at[:, rows(owner * d4, d4)],
                                     xqsem.at[0 if owner is t else 1])

    def x_quarter_send(owner):
        part = x.at[:, rows(owner * d4, d4)]
        return remote(part, part, xqsem.at[2 if owner is t else 3], xqsem.at[4 if owner is t else 5], (t, 0))

    def three(sem):
        part = x.at[:, pl.ds(0, 3 * d4)]
        return pltpu.make_async_copy(part, part, sem)

    @pl.when(c == 0)
    def _():
        for n in range(2):
            left_load(n)
        for n in range(2):
            right_load(n)
        for n in range(2):
            own_load(n).start()
        for n in range(2):
            left_update(n)
        for n in range(3):
            up_out(n).start()
        own[0]().start()
        for n in range(8):
            right_update(n)
        own[1]().start()
        base_loads(0, 0)
        base_loads(1, 1)
        x_quarter_send(t).wait_recv()

    @pl.when(c == 1)
    def _():
        x_quarter(t).start()
        for owner in others:
            x_quarter(owner).start()
        for n in range(2):
            own_load(n).start()
        base_loads(0, 0)
        base_loads(1, 1)
        x_quarter(t).wait()
        x_quarter_send(t).start()
        three(xqsem.at[1]).wait()
        for owner in others:
            x_quarter_send(owner).start()
        up_in(t).wait_recv()
        own[1]().wait_recv()

    own_load(0).wait()
    own_merge(0)
    own_store(0).start()

    def first_part(j, carry):
        @pl.when(j >= 2)
        def _():
            own_store(j - 2).wait()

        @pl.when(j + 2 < nb)
        def _():
            own_load(j + 2).start()
        own_load(j + 1).wait()
        own_dot(j)
        own_merge(j + 1)
        own_store(j + 1).start()

        def turn(n, *calls):
            @pl.when((c == 0) & (j == n * nb // 16))
            def _():
                for call in calls:
                    call()

        for n in range(2):
            turn(1 + n, functools.partial(right_update, 8 + n))
        turn(3, *[lambda n=n: dn_out(n).start() for n in range(3)], lambda: own[3]().start())
        for n in range(4):
            turn(4 + n, functools.partial(left_update, 2 + 2 * n), functools.partial(left_update, 3 + 2 * n))
        turn(8, lambda: own[2]().start())
        for n in range(3):
            turn((9, 10, 14)[n], lambda n=n: up_in(others[n]).wait_recv(), lambda n=n: pass_up(n).start())
        return carry

    lax.fori_loop(0, nb - 1, first_part, 0)
    own_dot(nb - 1)
    for j in range(nb - 3, nb):
        own_store(j).wait()

    @pl.when(c == 0)
    def _():
        own[1]().wait_send()
        three(xqsem.at[5]).wait()

    @pl.when(c == 1)
    def _():
        for owner in others:
            up_in(owner).wait_recv()

    up_wait(0)
    merge_up(0, 0)
    keep_rows(0)

    def tile_turn(r):
        @pl.when(r < nb)
        def _():
            up_store(r, r % RING)

        @pl.when(r >= nb)
        def _():
            merged_store(r, r % RING).start()

        @pl.when((r >= 1) & (r <= nb))
        def _():
            up_store_wait((r + 2) % RING)

        @pl.when(r > nb)
        def _():
            merged_store(r - 1, (r + 2) % RING).wait()

        @pl.when(r + 2 < 2 * nb)
        def _():
            base_loads(r + 2, (r + 2) % RING)

        @pl.when(r + 2 >= 2 * nb)
        def _():
            merged_load(r + 2 - 2 * nb, (r + 2) % RING).start()

        @pl.when(r + 1 < nb)
        def _():
            up_wait((r + 1) % RING)

        @pl.when(r + 1 >= nb)
        def _():
            merged_load(0, (r + 1) % RING).wait()

    def first_up(r, carry):
        @pl.when(r == nb // 2)
        def _():
            @pl.when(c == 0)
            def _():
                for n in range(3):
                    dn_in(others[n]).wait_recv()
                    pass_dn(n).start()
        tile_turn(r)
        other_parts(r % RING, r)
        merge_up((r + 1) % RING, r + 1)
        return carry

    lax.fori_loop(0, nb - 1, first_up, 0)

    @pl.when(c == 0)
    def _():
        for n in range(3):
            up_out(n).wait_send()
            dn_out(n).wait_send()
            pass_up(n).wait_send()
            pass_dn(n).wait_send()
        for n in (0, 2, 3):
            own[n]().wait_send()

    @pl.when(c == 1)
    def _():
        for owner in range(4):
            dn_in(owner).wait_recv()
        own[2]().wait_recv()

    tile_turn(nb - 1)
    other_parts((nb - 1) % RING, nb - 1)
    merge_dn(nb % RING, 0)

    def x_turn(k, r):
        @pl.when((k + 1 < nc) & (c == 0) & (r == nb))
        def _():
            pl.semaphore_signal(xfree, inc=1, device_id=(t, 1), device_id_type=MESH)

        @pl.when((k + 1 < nc) & (c == 1) & (r == nb))
        def _():
            @pl.when(k == 0)
            def _():
                x_quarter_send(t).wait_send()
                three(xqsem.at[3]).wait()

            @pl.when(k >= 1)
            def _():
                x_send().wait_send()
            x_load(k + 1).start()

        @pl.when((k + 1 < nc) & (c == 1) & (r == nb + 2))
        def _():
            x_load(k + 1).wait()
            pl.semaphore_wait(xfree, 1)
            x_send().start()

        @pl.when((k >= 1) & (r == 0))
        def _():
            @pl.when(c == 0)
            def _():
                x_send().wait_recv()
            keep_rows(k)

    def first_dn(r, carry):
        x_turn(0, r)
        tile_turn(r)
        dot_dn(r % RING, r % 2)
        merge_dn((r + 1) % RING, r + 1 - nb)
        swap(r - nb).start()
        stages(r)
        return carry

    lax.fori_loop(nb, 2 * nb - 1, first_dn, 0)

    def step(s, carry):
        k, r = s // (2 * nb), s % (2 * nb)
        x_turn(k, r)

        @pl.when(s == 2 * nb - 1)
        def _():
            tile_turn(2 * nb - 1)

        @pl.when(s == 2 * nb)
        def _():
            merged_store(2 * nb - 1, (2 * nb - 1) % RING).wait()

        @pl.when(s >= 2 * nb)
        def _():
            @pl.when(s + 2 < 2 * nb * nc)
            def _():
                merged_load((s + 2) % (2 * nb), (s + 2) % RING).start()

            @pl.when(s > 2 * nb)
            def _():
                merged_load(0, s % RING).wait()

        @pl.when(r < nb)
        def _():
            dot_up(s % RING, r)

        @pl.when(r >= nb)
        def _():
            dot_dn(s % RING, s % 2)
            swap(k * nb + r - nb).start()
        stages(s)
        return carry

    lax.fori_loop(2 * nb - 1, 2 * nb * nc, step, 0)

    def drain(s, carry):
        stages(s)
        return carry

    lax.fori_loop(2 * nb * nc, 2 * (total - 1) + nb + LAG[-1] + 1, drain, 0)

    @pl.when(c == 1)
    def _():
        x_send().wait_send()
        for n in range(3):
            part = hid.at[pl.ds(0, (nc - 1) * mq), :]
            pltpu.make_async_copy(part, part, fsem.at[n]).wait()
        pltpu.make_async_copy(near, near, fsem.at[3]).wait()


def fused_mlp(base_up, base_down, factors, learn_rate, prompts):
    tokens, d = prompts.shape[1:]
    fh = base_up.shape[2] // 2
    nb = fh // TILE
    w = d // nb
    m = min(CHUNK, tokens)
    nc = tokens // m
    rank = factors[0].shape[3]
    dims = (m, nc, nb, d, fh, w)
    dma = pltpu.SemaphoreType.DMA
    anywhere = pl.BlockSpec(memory_space=pl.ANY)
    hid, tail, near, _ = pl.pallas_call(
        functools.partial(mlp_kernel, dims),
        out_shape=(jax.ShapeDtypeStruct((tokens, d), BF16), jax.ShapeDtypeStruct((m // 4, d), BF16),
                   jax.ShapeDtypeStruct((m // 4, d), BF16), jax.ShapeDtypeStruct((2 * nb, d, TILE), BF16)),
        in_specs=[anywhere] * 10 + [pl.BlockSpec(memory_space=pltpu.SMEM), anywhere],
        out_specs=(anywhere,) * 4,
        scratch_shapes=[
            pltpu.VMEM((2, 2, d // 8, rank), F32),
            pltpu.VMEM((2, 2, rank, d // 8), F32),
            pltpu.VMEM((fh, rank), BF16),
            pltpu.VMEM((m, d), BF16),
            pltpu.VMEM((m, fh), BF16),
            pltpu.VMEM((RING, d, TILE), BF16),
            pltpu.VMEM((d, rank), BF16),
            pltpu.VMEM((rank, fh), BF16),
            pltpu.VMEM((fh, rank), BF16),
            pltpu.VMEM((rank, d), BF16),
            pltpu.VMEM((2, m, w), F32),
            pltpu.VMEM((4, m // 2, w), F32),
            pltpu.VMEM((nb, m // 2, w), F32),
            pltpu.VMEM((nb, m // 4, w), F32),
            pltpu.VMEM((nb, m // 8, w), F32),
            pltpu.VMEM((nb, m // 4, w), BF16),
            pltpu.VMEM((2, m // 8, d), BF16),
            dma((RING,)), dma((RING,)), dma((2,)), dma((2,)), dma((4,)), dma((4,)), dma((18,)), dma((10,)), dma((3,)), dma((6,)),
            dma((2,)), dma((4,)), dma((nb,)), dma((nb,)), dma((nb,)), dma((nb,)), dma((nb,)), dma((nb,)),
            dma((nb,)), dma((nb,)), dma((4,)),
            pltpu.SemaphoreType.REGULAR, pltpu.SemaphoreType.REGULAR,
            pltpu.SemaphoreType.REGULAR, pltpu.SemaphoreType.REGULAR,
        ],
        compiler_params=pltpu.CompilerParams(has_side_effects=True, vmem_limit_bytes=67043328),
        name='mlp_ring',
    )(base_up, base_down, *factors, learn_rate, prompts)
    return hid, tail, near


def finish_kernel(dims, hid, tail, near, a_up, a_up_g, b_up, b_up_g, a_dn, a_dn_g, b_dn, b_dn_g, rate,
                  out, a_up_n, b_up_n, a_dn_n, b_dn_n, buf, left, right, left_n, right_n, isem, osem, lsem, rsem, lnsem, rnsem):
    tokens, d, m, step = dims
    t = lax.axis_index('tp')
    c = lax.axis_index('pool')
    xb, yb = t % 2, t // 2
    mq = m // 4
    head = tokens - m
    slots = buf.shape[0]
    ahead = slots // 2
    size = d // 8

    lefts = [(a_up, a_up_g, a_up_n, q) for q in range(2)] + [(a_dn, a_dn_g, a_dn_n, q) for q in range(8)]
    rights = [(b_dn, b_dn_g, b_dn_n, q) for q in range(2)] + [(b_up, b_up_g, b_up_n, q) for q in range(8)]

    def left_piece(ref, q):
        return ref.at[0, 0, pl.ds(q * size, size), :]

    def right_piece(ref, q):
        return ref.at[0, 0, :, pl.ds(q * size, size)]

    def left_store(n, slot):
        return pltpu.make_async_copy(left_n.at[slot], left_piece(lefts[n][2], lefts[n][3]), lnsem.at[slot])

    def right_store(n, slot):
        return pltpu.make_async_copy(right_n.at[slot], right_piece(rights[n][2], rights[n][3]), rnsem.at[slot])

    @pl.when(c == 1)
    def _():
        moves = [(hid, q * step, q * step) for q in range(head // step)]
        moves += [(near, q * step, head + xb * mq + q * step) for q in range(mq // step)]
        moves += [(tail, q * step, head + 2 * mq + yb * mq + q * step) for q in range(mq // step)]

        def load(n):
            src, start, _ = moves[n]
            return pltpu.make_async_copy(src.at[pl.ds(start, step), :], buf.at[n % slots], isem.at[n % slots])

        def store(n):
            start = moves[n][2]
            return pltpu.make_async_copy(buf.at[n % slots], out.at[0, pl.ds(pl.multiple_of(start, step), step), :], osem.at[n % slots])

        for n in range(ahead):
            load(n).start()
        left_n[0] = jnp.zeros_like(left_n[0])
        right_n[0] = jnp.zeros_like(right_n[0])
        for n in range(len(moves)):
            load(n).wait()
            store(n).start()
            if n < 10:
                left_store(n, 0).start()
                right_store(n, 0).start()
            if n >= ahead:
                store(n - ahead).wait()
            if n + ahead < len(moves):
                load(n + ahead).start()
        for n in range(len(moves) - ahead, len(moves)):
            store(n).wait()
        for n in range(10):
            left_store(n, 0).wait()
            right_store(n, 0).wait()

    @pl.when(c == 0)
    def _():
        def left_load(n):
            for side in range(2):
                pltpu.make_async_copy(left_piece(lefts[n][side], lefts[n][3]), left.at[n % 2, side], lsem.at[n % 2]).start()

        def right_load(n):
            for side in range(2):
                pltpu.make_async_copy(right_piece(rights[n][side], rights[n][3]), right.at[n % 2, side], rsem.at[n % 2]).start()

        def blank(n):
            return pltpu.make_async_copy(buf.at[0], out.at[0, pl.ds(n * step, step), :], osem.at[0])

        for n in range(2):
            left_load(n)
            right_load(n)
        buf[0] = jnp.zeros_like(buf[0])
        blanks = tokens // step
        for n in range(10):
            pltpu.make_async_copy(left.at[n % 2], left.at[n % 2], lsem.at[n % 2]).wait()
            pltpu.make_async_copy(right.at[n % 2], right.at[n % 2], rsem.at[n % 2]).wait()
            if n >= 2:
                left_store(n - 2, n % 2).wait()
                right_store(n - 2, n % 2).wait()
            left_n[n % 2] = left[n % 2, 0] - rate[0] * left[n % 2, 1]
            right_n[n % 2] = right[n % 2, 0] - rate[0] * right[n % 2, 1]
            left_store(n, n % 2).start()
            right_store(n, n % 2).start()
            if n + 2 < 10:
                left_load(n + 2)
                right_load(n + 2)
            for q in range(n * blanks // 10, (n + 1) * blanks // 10):
                blank(q).start()
        for n in range(8, 10):
            left_store(n, n % 2).wait()
            right_store(n, n % 2).wait()
        for q in range(blanks):
            blank(q).wait()


def finish(hid, tail, near, factors, learn_rate, m):
    tokens, d = hid.shape
    rank = factors[0].shape[3]
    step = min(64, m // 4)
    dma = pltpu.SemaphoreType.DMA
    anywhere = pl.BlockSpec(memory_space=pl.ANY)
    return pl.pallas_call(
        functools.partial(finish_kernel, (tokens, d, m, step)),
        out_shape=(jax.ShapeDtypeStruct((1, tokens, d), BF16),) + tuple(jax.ShapeDtypeStruct(f.shape, F32) for f in factors[::2]),
        in_specs=[anywhere] * 11 + [pl.BlockSpec(memory_space=pltpu.SMEM)],
        out_specs=(anywhere,) * 5,
        scratch_shapes=[
            pltpu.VMEM((8, step, d), BF16),
            pltpu.VMEM((2, 2, d // 8, rank), F32),
            pltpu.VMEM((2, 2, rank, d // 8), F32),
            pltpu.VMEM((2, d // 8, rank), F32),
            pltpu.VMEM((2, rank, d // 8), F32),
            dma((8,)), dma((8,)), dma((2,)), dma((2,)), dma((2,)), dma((2,)),
        ],
        compiler_params=pltpu.CompilerParams(vmem_limit_bytes=67043328),
        cost_estimate=pl.CostEstimate(flops=20_000_000_000, bytes_accessed=70_000_000, transcendentals=0),
        name='finish',
    )(hid, tail, near, *factors, learn_rate)


def solution(mesh):
    left_spec = P('pool', None, 'tp', None)
    right_spec = P('pool', None, None, 'tp')
    prompt_spec = P('pool', None, None)

    def local_step(base_up, base_down, up_left, up_right, down_left, down_right, grad_up_left, grad_up_right, grad_down_left, grad_down_right, learn_rate, prompts):
        t = lax.axis_index('tp')
        xb, yb = t % 2, t // 2
        factors = (up_left, grad_up_left, up_right, grad_up_right, down_left, grad_down_left, down_right, grad_down_right)
        m = min(CHUNK, prompts.shape[1])
        hid, tail, near = fused_mlp(base_up, base_down, factors, learn_rate, prompts)
        from_x = lax.ppermute(tail, ('tp', 'pool'), [(2 * n, 2 * (n ^ 1) + 1) for n in range(4)])
        from_y = lax.ppermute(tail, ('tp', 'pool'), [(2 * n + 1, 2 * (n ^ 2) + 1) for n in range(4)])
        hidden_out, new_up_left, new_up_right, new_down_left, new_down_right = finish(hid, tail, near, factors, learn_rate, m)
        start = hid.shape[0] - m
        hidden_out = lax.dynamic_update_slice(hidden_out, from_x[None], (0, start + (1 - xb) * (m // 4), 0))
        hidden_out = lax.dynamic_update_slice(hidden_out, from_y[None], (0, start + m // 2 + (1 - yb) * (m // 4), 0))
        return new_up_left, new_up_right, new_down_left, new_down_right, hidden_out

    return jax.shard_map(local_step, mesh=mesh,
                         in_specs=(P(None, None, 'tp'), P(None, 'tp', None), left_spec, right_spec, left_spec, right_spec, left_spec, right_spec, left_spec, right_spec, P(None), prompt_spec),
                         out_specs=(left_spec, right_spec, left_spec, right_spec, prompt_spec),
                         check_vma=False)
```

```python
import functools

import jax
import jax.numpy as jnp
from jax import lax
from jax.experimental import pallas as pl
from jax.experimental.pallas import tpu as pltpu
from jax.sharding import PartitionSpec as P

CHUNK = 512
TILE = 256
RING = 3
PIECE = 1024
LAG = (2, 4, 7, 23)
BF16 = jnp.bfloat16
F32 = jnp.float32
MESH = pl.DeviceIdType.MESH


def mlp_kernel(dims, base_up, base_dn, a_up, a_up_g, b_up, b_up_g, a_dn, a_dn_g, b_dn, b_dn_g, rate, prompts, hid, tail, near, wm,
               left, right, far_a, x, u, wb, aup, bup, adn, bdn, pb, rx0, s1, rx1, rx2, ob, res,
               wsem, osem, lsem, rsem, qload, qstore, asend, arecv, xsem, xqsem, s0, r0, ss1, rs1, ss2, rs2, ss3, rs3, ss4, ss5, fsem,
               xfree, cr1, cr2, cr3):
    m, nc, nb, d, fh, w = dims
    total = nc * nb
    ring = nb
    halves = w // TILE
    mh, mq, me = m // 2, m // 4, m // 8
    d4 = d // 4
    rank = aup.shape[1]
    t = lax.axis_index('tp')
    c = lax.axis_index('pool')
    trainer, generator = c == 0, c == 1
    period = 2 * nb
    xb, yb = t % 2, t // 2
    near_x, near_y = t + 1 - 2 * xb, t + 2 - 4 * yb
    b1 = (1 - c) * xb + c * yb
    b2 = c * xb + (1 - c) * yb
    p1 = (1 - c) * near_x + c * near_y
    p2 = c * near_x + (1 - c) * near_y
    others = (near_x, near_y, 3 - t)

    def rows(start, size):
        return pl.ds(pl.multiple_of(start, size), size)

    def remote(src, dst, send, recv, device):
        return pltpu.make_async_remote_copy(src_ref=src, dst_ref=dst, send_sem=send, recv_sem=recv,
                                            device_id=device, device_id_type=MESH)

    def spread(src, dst, sem):
        size = min(PIECE, src.shape[0])
        for start in range(0, src.shape[0], size):
            pltpu.make_async_copy(src.at[pl.ds(start, size)], dst.at[pl.ds(start, size)], sem).start()

    def base_loads(r, slot):
        @pl.when(r < nb)
        def _():
            for q in others:
                spread(base_up.at[0, rows(q * d4, d4), rows(c * fh + r * TILE, TILE)],
                       wb.at[slot, rows(q * d4, d4), :], wsem.at[slot])

        @pl.when(r >= nb)
        def _():
            for h in range(halves):
                spread(base_dn.at[0, rows(c * fh, fh), rows((r - nb) * w + h * TILE, TILE)],
                       wb.at[slot, pl.ds(h * fh, fh), :], wsem.at[slot])

    def up_wait(slot):
        part = wb.at[slot, pl.ds(0, 3 * d4), :]
        pltpu.make_async_copy(part, part, wsem.at[slot]).wait()

    def up_store(r, slot):
        for q in others:
            spread(wb.at[slot, rows(q * d4, d4), :], wm.at[r, rows(q * d4, d4), :], osem.at[slot])

    def up_store_wait(slot):
        part = wb.at[slot, pl.ds(0, 3 * d4), :]
        pltpu.make_async_copy(part, part, osem.at[slot]).wait()

    def merged_load(r, slot):
        return pltpu.make_async_copy(wm.at[r], wb.at[slot], wsem.at[slot])

    def merged_store(r, slot):
        return pltpu.make_async_copy(wb.at[slot], wm.at[r], osem.at[slot])

    piece = min(512, d4)

    def merge_up(slot, j):
        cols = bup[:, rows(j * TILE, TILE)]
        for q in others:
            for n in range(d4 // piece):
                part = rows(q * d4 + n * piece, piece)
                delta = jnp.dot(aup[part, :], cols, preferred_element_type=F32).astype(BF16)
                wb[slot, part, :] = wb[slot, part, :] + delta

    def own_rows(j):
        return wb.at[RING - 1, rows((j % 4) * d4, d4), :]

    def own_load(j):
        spread(base_up.at[0, rows(t * d4, d4), rows(c * fh + j * TILE, TILE)], own_rows(j), qload.at[j % 4])

    def own_store(j):
        spread(own_rows(j), wm.at[j, rows(t * d4, d4), :], qstore.at[j % 4])

    def own_wait(j, sem):
        pltpu.make_async_copy(own_rows(j), own_rows(j), sem.at[j % 4]).wait()

    def own_merge(j):
        cols = bup[:, rows(j * TILE, TILE)]
        for n in range(d4 // piece):
            part = rows((j % 4) * d4 + n * piece, piece)
            delta = jnp.dot(aup[rows(t * d4 + n * piece, piece), :], cols, preferred_element_type=F32).astype(BF16)
            wb[RING - 1, part, :] = wb[RING - 1, part, :] + delta

    def own_dot(j):
        pre = jnp.dot(x[:, rows(t * d4, d4)], wb[RING - 1, rows((j % 4) * d4, d4), :], preferred_element_type=F32)
        s1[j, :, pl.ds(0, TILE)] = pre[:mh]
        s1[j, :, pl.ds(TILE, TILE)] = pre[mh:]

    def other_parts(slot, j):
        pre = sum(jnp.dot(x[:, rows(q * d4, d4)], wb[slot, rows(q * d4, d4), :], preferred_element_type=F32) for q in others)
        top = pre[:mh] + s1[j, :, pl.ds(0, TILE)]
        low = pre[mh:] + s1[j, :, pl.ds(TILE, TILE)]
        u[pl.ds(0, mh), rows(j * TILE, TILE)] = jax.nn.gelu(top, approximate=True).astype(BF16)
        u[pl.ds(mh, mh), rows(j * TILE, TILE)] = jax.nn.gelu(low, approximate=True).astype(BF16)

    def merge_dn(slot, i):
        for h in range(halves):
            cols = bdn[:, rows(i * w + h * TILE, TILE)]
            for q in range(fh // piece):
                delta = jnp.dot(adn[pl.ds(q * piece, piece), :], cols, preferred_element_type=F32).astype(BF16)
                part = pl.ds(h * fh + q * piece, piece)
                wb[slot, part, :] = wb[slot, part, :] + delta

    def dot_up(slot, j):
        pre = jnp.dot(x[...], wb[slot], preferred_element_type=F32)
        u[:, rows(j * TILE, TILE)] = jax.nn.gelu(pre, approximate=True).astype(BF16)

    def dot_dn(slot, buf):
        for h in range(halves):
            pb[buf, :, pl.ds(h * TILE, TILE)] = jnp.dot(u[...], wb[slot, pl.ds(h * fh, fh), :],
                                                        preferred_element_type=F32)

    def swap(g):
        return remote(pb.at[g % 2, rows((1 - c) * mh, mh), :], rx0.at[g % 4], s0.at[g % 2], r0.at[g % 4], (t, 1 - c))

    def first(g):
        return remote(s1.at[g % ring, rows((1 - b1) * mq, mq), :], rx1.at[g % ring],
                      ss1.at[g % ring], rs1.at[g % ring], (p1, c))

    def second(g):
        return remote(s1.at[g % ring, rows(b1 * mq + (1 - b2) * me, me), :], rx2.at[g % ring],
                      ss2.at[g % ring], rs2.at[g % ring], (p2, c))

    def gather(g):
        half = ob.at[g % ring, rows(b2 * me, me), :]
        return remote(half, half, ss3.at[g % ring], rs3.at[g % ring], (p2, c))

    def final_place(g):
        return hid.at[rows((g // nb) * m + c * mh + b1 * mq, mq), rows((g % nb) * w, w)]

    def final_far(g):
        return remote(ob.at[g % ring], final_place(g), ss4.at[g % ring], fsem.at[1 + c], (p1, 1))

    def final_near(g):
        return remote(ob.at[g % ring], final_place(g), ss5.at[g % ring], fsem.at[0], (t, 1))

    def final_local(g):
        return pltpu.make_async_copy(ob.at[g % ring], final_place(g), ss5.at[g % ring])

    def stage_a(g):
        slot = g % ring
        swap(g).wait_send()
        swap(g).wait_recv()
        s1[slot] = pb[g % 2, rows(c * mh, mh), :] + rx0[g % 4]

        @pl.when(g >= ring)
        def _():
            pl.semaphore_wait(cr1, 1)
        first(g).start()

    def stage_b(g):
        slot = g % ring
        keep = rows(b1 * mq, mq)
        first(g).wait_recv()
        s1[slot, keep, :] = s1[slot, keep, :] + rx1[slot]

        @pl.when(g + ring < total)
        def _():
            pl.semaphore_signal(cr1, inc=1, device_id=(p1, c), device_id_type=MESH)

        @pl.when(g >= ring)
        def _():
            pl.semaphore_wait(cr2, 1)
        second(g).start()

    def stage_c(g):
        slot = g % ring
        keep = rows(b1 * mq + b2 * me, me)
        second(g).wait_recv()
        first(g).wait_send()
        held = res[(g // nb) % 2, :, rows((g % nb) * w, w)].astype(F32)
        ob[slot, rows(b2 * me, me), :] = (held + (s1[slot, keep, :] + rx2[slot])).astype(BF16)

        @pl.when(g + ring < total)
        def _():
            pl.semaphore_signal(cr2, inc=1, device_id=(p2, c), device_id_type=MESH)

        @pl.when(g >= ring)
        def _():
            pl.semaphore_wait(cr3, 1)
        gather(g).start()

    def tail_local(g):
        return pltpu.make_async_copy(ob.at[g % ring], tail.at[:, rows((g % nb) * w, w)], ss4.at[g % ring])

    def tail_near(g):
        return remote(ob.at[g % ring], near.at[:, rows((g % nb) * w, w)], ss5.at[g % ring], fsem.at[3], (t, 1))

    def stage_d(g):
        gather(g).wait_recv()
        second(g).wait_send()

        @pl.when(g < total - nb)
        def _():
            final_far(g).start()

            @pl.when(trainer)
            def _():
                final_near(g).start()

            @pl.when(generator)
            def _():
                final_local(g).start()

        @pl.when(g >= total - nb)
        def _():
            tail_local(g).start()

            @pl.when(trainer)
            def _():
                tail_near(g).start()

    def stage_e(g):
        gather(g).wait_send()

        @pl.when(g < total - nb)
        def _():
            final_far(g).wait_send()

            @pl.when(trainer)
            def _():
                final_near(g).wait_send()

            @pl.when(generator)
            def _():
                final_local(g).wait()

        @pl.when(g >= total - nb)
        def _():
            tail_local(g).wait()

            @pl.when(trainer)
            def _():
                tail_near(g).wait_send()

        @pl.when(g + ring < total)
        def _():
            pl.semaphore_signal(cr3, inc=1, device_id=(p2, c), device_id_type=MESH)

    def stages(s):
        before = s - 1
        r = before % period

        @pl.when((r >= nb) & (before < period * nc))
        def _():
            stage_a((before // period) * nb + r - nb)
        for lag, stage in zip(LAG, (stage_b, stage_c, stage_d, stage_e)):
            late = s - nb - lag

            @pl.when((late >= 0) & (late % 2 == 0) & (late < 2 * total))
            def _():
                stage(late // 2)

    def x_load(k):
        return pltpu.make_async_copy(prompts.at[0, rows(k * m, m), :], x, xsem.at[0])

    def x_send():
        return remote(x, x, xsem.at[1], xsem.at[2], (t, 0))

    def keep_rows(k):
        res[k % 2] = x[rows(c * mh + b1 * mq + b2 * me, me), :]

    def up_piece(owner):
        return aup.at[rows(owner * d4, d4), :]

    def dn_piece(owner):
        return bdn.at[:, rows(owner * d4, d4)]

    def up_out(n):
        return remote(up_piece(t), up_piece(t), asend.at[n], arecv.at[t], (others[n], 0))

    def dn_out(n):
        return remote(dn_piece(t), dn_piece(t), asend.at[3 + n], arecv.at[4 + t], (others[n], 0))

    def up_in(owner):
        return remote(up_piece(owner), up_piece(owner), asend.at[6], arecv.at[owner], (t, 1))

    def dn_in(owner):
        return remote(dn_piece(owner), dn_piece(owner), asend.at[7], arecv.at[4 + owner], (t, 1))

    def pass_up(n):
        return remote(up_piece(others[n]), up_piece(others[n]), asend.at[8 + n], arecv.at[others[n]], (t, 1))

    def pass_dn(n):
        return remote(dn_piece(others[n]), dn_piece(others[n]), asend.at[11 + n], arecv.at[4 + others[n]], (t, 1))

    far_b = u.at[pl.ds(0, rank), :]
    own = (
        lambda: remote(up_piece(t), up_piece(t), asend.at[14], arecv.at[t], (t, 1)),
        lambda: remote(far_b, bup, asend.at[15], arecv.at[8], (t, 1)),
        lambda: remote(far_a, adn, asend.at[16], arecv.at[9], (t, 1)),
        lambda: remote(dn_piece(t), dn_piece(t), asend.at[17], arecv.at[4 + t], (t, 1)),
    )

    size = d4 // 2
    lefts = [(a_up, a_up_g, q, aup, t * d4 + q * size) for q in range(2)]
    lefts += [(a_dn, a_dn_g, q, adn, q * size) for q in range(4)]
    lefts += [(a_dn, a_dn_g, 4 + q, far_a, q * size) for q in range(4)]
    rights = [(b_up, b_up_g, q, bup, q * size) for q in range(4)]
    rights += [(b_up, b_up_g, 4 + q, u, q * size) for q in range(4)]
    rights += [(b_dn, b_dn_g, q, bdn, t * d4 + q * size) for q in range(2)]

    def left_load(n):
        value, grad, q, _, _ = lefts[n]
        for side, src in enumerate((value, grad)):
            pltpu.make_async_copy(src.at[0, 0, pl.ds(q * size, size), :], left.at[n % 2, side], lsem.at[n % 2]).start()

    def right_load(n):
        value, grad, q, _, _ = rights[n]
        for side, src in enumerate((value, grad)):
            pltpu.make_async_copy(src.at[0, 0, :, pl.ds(q * size, size)], right.at[n % 2, side], rsem.at[n % 2]).start()

    def left_update(n):
        _, _, _, dst, start = lefts[n]
        pltpu.make_async_copy(left.at[n % 2], left.at[n % 2], lsem.at[n % 2]).wait()
        new = (left[n % 2, 0] - rate[0] * left[n % 2, 1]).astype(BF16)
        dst[rows(start, size), :] = new
        if n + 2 < len(lefts):
            left_load(n + 2)

    def right_update(n):
        _, _, _, dst, start = rights[n]
        pltpu.make_async_copy(right.at[n % 2], right.at[n % 2], rsem.at[n % 2]).wait()
        new = (right[n % 2, 0] - rate[0] * right[n % 2, 1]).astype(BF16)
        if dst is u:
            u[pl.ds(0, rank), rows(start, size)] = new
        else:
            dst[:, rows(start, size)] = new
        if n + 2 < len(rights):
            right_load(n + 2)

    def x_quarter(owner):
        return pltpu.make_async_copy(prompts.at[0, pl.ds(0, m), rows(owner * d4, d4)], x.at[:, rows(owner * d4, d4)],
                                     xqsem.at[0 if owner is t else 1])

    def x_quarter_send(owner):
        part = x.at[:, rows(owner * d4, d4)]
        return remote(part, part, xqsem.at[2 if owner is t else 3], xqsem.at[4 if owner is t else 5], (t, 0))

    def three(sem):
        part = x.at[:, pl.ds(0, 3 * d4)]
        return pltpu.make_async_copy(part, part, sem)

    @pl.when(trainer)
    def _():
        for n in range(2):
            left_load(n)
        for n in range(2):
            right_load(n)
        for n in range(2):
            own_load(n)
        for n in range(2):
            left_update(n)
        for n in range(3):
            up_out(n).start()
        own[0]().start()
        for n in range(8):
            right_update(n)
        own[1]().start()
        base_loads(0, 0)
        base_loads(1, 1)
        x_quarter_send(t).wait_recv()

    @pl.when(generator)
    def _():
        x_quarter(t).start()
        for owner in others:
            x_quarter(owner).start()
        for n in range(2):
            own_load(n)
        base_loads(0, 0)
        base_loads(1, 1)
        x_quarter(t).wait()
        x_quarter_send(t).start()
        three(xqsem.at[1]).wait()
        for owner in others:
            x_quarter_send(owner).start()
        up_in(t).wait_recv()
        own[1]().wait_recv()

    own_wait(0, qload)
    own_merge(0)
    own_store(0)

    def first_part(j, carry):
        @pl.when(j >= 2)
        def _():
            own_wait(j - 2, qstore)

        @pl.when(j + 2 < nb)
        def _():
            own_load(j + 2)
        own_wait(j + 1, qload)
        own_dot(j)
        own_merge(j + 1)
        own_store(j + 1)

        def turn(n, *calls):
            @pl.when((trainer) & (j == n * (nb - 1) // 16))
            def _():
                for call in calls:
                    call()

        for n in range(2):
            turn(1 + n, functools.partial(right_update, 8 + n))
        turn(3, *[lambda n=n: dn_out(n).start() for n in range(3)], lambda: own[3]().start())
        for n in range(4):
            turn(4 + n, functools.partial(left_update, 2 + 2 * n), functools.partial(left_update, 3 + 2 * n))
        turn(8, lambda: own[2]().start())
        for n in range(3):
            turn((9, 10, 14)[n], lambda n=n: up_in(others[n]).wait_recv(), lambda n=n: pass_up(n).start())
        return carry

    lax.fori_loop(0, nb - 1, first_part, 0)
    own_dot(nb - 1)
    for j in range(nb - 3, nb):
        own_wait(j, qstore)

    @pl.when(trainer)
    def _():
        own[1]().wait_send()
        three(xqsem.at[5]).wait()

    @pl.when(generator)
    def _():
        for owner in others:
            up_in(owner).wait_recv()

    up_wait(0)
    merge_up(0, 0)
    keep_rows(0)

    def tile_turn(r):
        @pl.when(r < nb)
        def _():
            up_store(r, r % RING)

        @pl.when(r >= nb)
        def _():
            spread(wb.at[r % RING], wm.at[r], osem.at[r % RING])

        @pl.when((r >= 1) & (r <= nb))
        def _():
            up_store_wait((r + 2) % RING)

        @pl.when(r > nb)
        def _():
            merged_store(r - 1, (r + 2) % RING).wait()

        @pl.when(r + 2 < period)
        def _():
            base_loads(r + 2, (r + 2) % RING)

        @pl.when(r + 2 >= period)
        def _():
            spread(wm.at[r + 2 - period], wb.at[(r + 2) % RING], wsem.at[(r + 2) % RING])

        @pl.when(r + 1 < nb)
        def _():
            up_wait((r + 1) % RING)

        @pl.when(r + 1 >= nb)
        def _():
            merged_load(0, (r + 1) % RING).wait()

    def first_up(r, carry):
        @pl.when(r == nb // 2)
        def _():
            @pl.when(trainer)
            def _():
                for n in range(3):
                    dn_in(others[n]).wait_recv()
                    pass_dn(n).start()
        tile_turn(r)
        other_parts(r % RING, r)
        merge_up((r + 1) % RING, r + 1)
        return carry

    lax.fori_loop(0, nb - 1, first_up, 0)

    @pl.when(trainer)
    def _():
        for n in range(3):
            up_out(n).wait_send()
            dn_out(n).wait_send()
            pass_up(n).wait_send()
            pass_dn(n).wait_send()
        for n in (0, 2, 3):
            own[n]().wait_send()

    @pl.when(generator)
    def _():
        for owner in range(4):
            dn_in(owner).wait_recv()
        own[2]().wait_recv()

    tile_turn(nb - 1)
    other_parts((nb - 1) % RING, nb - 1)
    merge_dn(nb % RING, 0)

    def x_turn(k, r):
        @pl.when((k + 1 < nc) & (trainer) & (r == nb))
        def _():
            pl.semaphore_signal(xfree, inc=1, device_id=(t, 1), device_id_type=MESH)

        @pl.when((k + 1 < nc) & (generator) & (r == nb))
        def _():
            @pl.when(k == 0)
            def _():
                x_quarter_send(t).wait_send()
                three(xqsem.at[3]).wait()

            @pl.when(k >= 1)
            def _():
                x_send().wait_send()
            x_load(k + 1).start()

        @pl.when((k + 1 < nc) & (generator) & (r == nb + 2))
        def _():
            x_load(k + 1).wait()
            pl.semaphore_wait(xfree, 1)
            x_send().start()

        @pl.when((k >= 1) & (r == 0))
        def _():
            @pl.when(trainer)
            def _():
                x_send().wait_recv()
            keep_rows(k)

    def first_dn(r, carry):
        x_turn(0, r)
        tile_turn(r)
        dot_dn(r % RING, r % 2)
        merge_dn((r + 1) % RING, r + 1 - nb)
        swap(r - nb).start()
        stages(r)
        return carry

    lax.fori_loop(nb, period - 1, first_dn, 0)

    def step(s, carry):
        k, r = s // period, s % period
        x_turn(k, r)

        @pl.when(s == period - 1)
        def _():
            tile_turn(period - 1)

        @pl.when(s == period)
        def _():
            merged_store(period - 1, (period - 1) % RING).wait()

        @pl.when(s >= period)
        def _():
            @pl.when(s + 2 < period * nc)
            def _():
                spread(wm.at[(s + 2) % period], wb.at[(s + 2) % RING], wsem.at[(s + 2) % RING])

            @pl.when(s > period)
            def _():
                merged_load(0, s % RING).wait()

        @pl.when(r < nb)
        def _():
            dot_up(s % RING, r)

        @pl.when(r >= nb)
        def _():
            dot_dn(s % RING, s % 2)
            swap(k * nb + r - nb).start()
        stages(s)
        return carry

    lax.fori_loop(period - 1, period * nc, step, 0)

    def drain(s, carry):
        stages(s)
        return carry

    lax.fori_loop(period * nc, 2 * (total - 1) + nb + LAG[-1] + 1, drain, 0)

    @pl.when(generator)
    def _():
        x_send().wait_send()
        for n in range(3):
            part = hid.at[pl.ds(0, (nc - 1) * mq), :]
            pltpu.make_async_copy(part, part, fsem.at[n]).wait()
        pltpu.make_async_copy(near, near, fsem.at[3]).wait()


def fused_mlp(base_up, base_down, factors, learn_rate, prompts):
    tokens, d = prompts.shape[1:]
    fh = base_up.shape[2] // 2
    nb = fh // TILE
    w = d // nb
    m = min(CHUNK, tokens)
    nc = tokens // m
    rank = factors[0].shape[3]
    dims = (m, nc, nb, d, fh, w)
    dma = pltpu.SemaphoreType.DMA
    anywhere = pl.BlockSpec(memory_space=pl.ANY)
    hid, tail, near, _ = pl.pallas_call(
        functools.partial(mlp_kernel, dims),
        out_shape=(jax.ShapeDtypeStruct((tokens, d), BF16), jax.ShapeDtypeStruct((m // 4, d), BF16),
                   jax.ShapeDtypeStruct((m // 4, d), BF16), jax.ShapeDtypeStruct((2 * nb, d, TILE), BF16)),
        in_specs=[anywhere] * 10 + [pl.BlockSpec(memory_space=pltpu.SMEM), anywhere],
        out_specs=(anywhere,) * 4,
        scratch_shapes=[
            pltpu.VMEM((2, 2, d // 8, rank), F32),
            pltpu.VMEM((2, 2, rank, d // 8), F32),
            pltpu.VMEM((fh, rank), BF16),
            pltpu.VMEM((m, d), BF16),
            pltpu.VMEM((m, fh), BF16),
            pltpu.VMEM((RING, d, TILE), BF16),
            pltpu.VMEM((d, rank), BF16),
            pltpu.VMEM((rank, fh), BF16),
            pltpu.VMEM((fh, rank), BF16),
            pltpu.VMEM((rank, d), BF16),
            pltpu.VMEM((2, m, w), F32),
            pltpu.VMEM((4, m // 2, w), F32),
            pltpu.VMEM((nb, m // 2, w), F32),
            pltpu.VMEM((nb, m // 4, w), F32),
            pltpu.VMEM((nb, m // 8, w), F32),
            pltpu.VMEM((nb, m // 4, w), BF16),
            pltpu.VMEM((2, m // 8, d), BF16),
            dma((RING,)), dma((RING,)), dma((2,)), dma((2,)), dma((4,)), dma((4,)), dma((18,)), dma((10,)), dma((3,)), dma((6,)),
            dma((2,)), dma((4,)), dma((nb,)), dma((nb,)), dma((nb,)), dma((nb,)), dma((nb,)), dma((nb,)),
            dma((nb,)), dma((nb,)), dma((4,)),
            pltpu.SemaphoreType.REGULAR, pltpu.SemaphoreType.REGULAR,
            pltpu.SemaphoreType.REGULAR, pltpu.SemaphoreType.REGULAR,
        ],
        compiler_params=pltpu.CompilerParams(has_side_effects=True, vmem_limit_bytes=67043328),
        name='mlp_ring',
    )(base_up, base_down, *factors, learn_rate, prompts)
    return hid, tail, near


def finish_kernel(dims, hid, tail, near, a_up, a_up_g, b_up, b_up_g, a_dn, a_dn_g, b_dn, b_dn_g, rate,
                  out, a_up_n, b_up_n, a_dn_n, b_dn_n, buf, left, right, left_n, right_n, isem, osem, lsem, rsem, lnsem, rnsem):
    tokens, d, m, step = dims
    t = lax.axis_index('tp')
    c = lax.axis_index('pool')
    xb, yb = t % 2, t // 2
    mq = m // 4
    head = tokens - m
    slots = buf.shape[0]
    ahead = slots // 2
    size = d // 8

    lefts = [(a_up, a_up_g, a_up_n, q) for q in range(2)] + [(a_dn, a_dn_g, a_dn_n, q) for q in range(8)]
    rights = [(b_dn, b_dn_g, b_dn_n, q) for q in range(2)] + [(b_up, b_up_g, b_up_n, q) for q in range(8)]

    def left_piece(ref, q):
        return ref.at[0, 0, pl.ds(q * size, size), :]

    def right_piece(ref, q):
        return ref.at[0, 0, :, pl.ds(q * size, size)]

    def left_store(n, slot):
        return pltpu.make_async_copy(left_n.at[slot], left_piece(lefts[n][2], lefts[n][3]), lnsem.at[slot])

    def right_store(n, slot):
        return pltpu.make_async_copy(right_n.at[slot], right_piece(rights[n][2], rights[n][3]), rnsem.at[slot])

    @pl.when(c == 1)
    def _():
        moves = [(hid, q * step, q * step) for q in range(head // step)]
        moves += [(near, q * step, head + xb * mq + q * step) for q in range(mq // step)]
        moves += [(tail, q * step, head + 2 * mq + yb * mq + q * step) for q in range(mq // step)]

        def load(n):
            src, start, _ = moves[n]
            return pltpu.make_async_copy(src.at[pl.ds(start, step), :], buf.at[n % slots], isem.at[n % slots])

        def store(n):
            start = moves[n][2]
            return pltpu.make_async_copy(buf.at[n % slots], out.at[0, pl.ds(pl.multiple_of(start, step), step), :], osem.at[n % slots])

        for n in range(ahead):
            load(n).start()
        left_n[0] = jnp.zeros_like(left_n[0])
        right_n[0] = jnp.zeros_like(right_n[0])
        for n in range(len(moves)):
            load(n).wait()
            store(n).start()
            if n < len(lefts):
                left_store(n, 0).start()
                right_store(n, 0).start()
            if n >= ahead:
                store(n - ahead).wait()
            if n + ahead < len(moves):
                load(n + ahead).start()
        for n in range(len(moves) - ahead, len(moves)):
            store(n).wait()
        for n in range(len(lefts)):
            left_store(n, 0).wait()
            right_store(n, 0).wait()

    @pl.when(c == 0)
    def _():
        def left_load(n):
            for side in range(2):
                pltpu.make_async_copy(left_piece(lefts[n][side], lefts[n][3]), left.at[n % 2, side], lsem.at[n % 2]).start()

        def right_load(n):
            for side in range(2):
                pltpu.make_async_copy(right_piece(rights[n][side], rights[n][3]), right.at[n % 2, side], rsem.at[n % 2]).start()

        def blank(n):
            return pltpu.make_async_copy(buf.at[0], out.at[0, pl.ds(n * step, step), :], osem.at[0])

        for n in range(2):
            left_load(n)
            right_load(n)
        buf[0] = jnp.zeros_like(buf[0])
        blanks = tokens // step
        for n in range(10):
            pltpu.make_async_copy(left.at[n % 2], left.at[n % 2], lsem.at[n % 2]).wait()
            pltpu.make_async_copy(right.at[n % 2], right.at[n % 2], rsem.at[n % 2]).wait()
            if n >= 2:
                left_store(n - 2, n % 2).wait()
                right_store(n - 2, n % 2).wait()
            left_n[n % 2] = left[n % 2, 0] - rate[0] * left[n % 2, 1]
            right_n[n % 2] = right[n % 2, 0] - rate[0] * right[n % 2, 1]
            left_store(n, n % 2).start()
            right_store(n, n % 2).start()
            if n + 2 < 10:
                left_load(n + 2)
                right_load(n + 2)
            for q in range(n * blanks // 10, (n + 1) * blanks // 10):
                blank(q).start()
        for n in range(8, 10):
            left_store(n, n % 2).wait()
            right_store(n, n % 2).wait()
        for q in range(blanks):
            blank(q).wait()


def finish(hid, tail, near, factors, learn_rate, m):
    tokens, d = hid.shape
    rank = factors[0].shape[3]
    step = min(64, m // 4)
    dma = pltpu.SemaphoreType.DMA
    anywhere = pl.BlockSpec(memory_space=pl.ANY)
    return pl.pallas_call(
        functools.partial(finish_kernel, (tokens, d, m, step)),
        out_shape=(jax.ShapeDtypeStruct((1, tokens, d), BF16),) + tuple(jax.ShapeDtypeStruct(f.shape, F32) for f in factors[::2]),
        in_specs=[anywhere] * 11 + [pl.BlockSpec(memory_space=pltpu.SMEM)],
        out_specs=(anywhere,) * 5,
        scratch_shapes=[
            pltpu.VMEM((8, step, d), BF16),
            pltpu.VMEM((2, 2, d // 8, rank), F32),
            pltpu.VMEM((2, 2, rank, d // 8), F32),
            pltpu.VMEM((2, d // 8, rank), F32),
            pltpu.VMEM((2, rank, d // 8), F32),
            dma((8,)), dma((8,)), dma((2,)), dma((2,)), dma((2,)), dma((2,)),
        ],
        compiler_params=pltpu.CompilerParams(vmem_limit_bytes=67043328),
        cost_estimate=pl.CostEstimate(flops=20_000_000_000, bytes_accessed=70_000_000, transcendentals=0),
        name='finish',
    )(hid, tail, near, *factors, learn_rate)


def solution(mesh):
    left_spec = P('pool', None, 'tp', None)
    right_spec = P('pool', None, None, 'tp')
    prompt_spec = P('pool', None, None)

    def local_step(base_up, base_down, up_left, up_right, down_left, down_right, grad_up_left, grad_up_right, grad_down_left, grad_down_right, learn_rate, prompts):
        t = lax.axis_index('tp')
        xb, yb = t % 2, t // 2
        factors = (up_left, grad_up_left, up_right, grad_up_right, down_left, grad_down_left, down_right, grad_down_right)
        m = min(CHUNK, prompts.shape[1])
        hid, tail, near = fused_mlp(base_up, base_down, factors, learn_rate, prompts)
        from_x = lax.ppermute(tail, ('tp', 'pool'), [(2 * n, 2 * (n ^ 1) + 1) for n in range(4)])
        from_y = lax.ppermute(tail, ('tp', 'pool'), [(2 * n + 1, 2 * (n ^ 2) + 1) for n in range(4)])
        hidden_out, new_up_left, new_up_right, new_down_left, new_down_right = finish(hid, tail, near, factors, learn_rate, m)
        start = hid.shape[0] - m
        hidden_out = lax.dynamic_update_slice(hidden_out, from_x[None], (0, start + (1 - xb) * (m // 4), 0))
        hidden_out = lax.dynamic_update_slice(hidden_out, from_y[None], (0, start + m // 2 + (1 - yb) * (m // 4), 0))
        return new_up_left, new_up_right, new_down_left, new_down_right, hidden_out

    return jax.shard_map(local_step, mesh=mesh,
                         in_specs=(P(None, None, 'tp'), P(None, 'tp', None), left_spec, right_spec, left_spec, right_spec, left_spec, right_spec, left_spec, right_spec, P(None), prompt_spec),
                         out_specs=(left_spec, right_spec, left_spec, right_spec, prompt_spec),
                         check_vma=False)
```
